32 devices in a mesh: sector: 8 (over z, core), cap: 4 (over y, x).
Axes of the slice: x: 2, y: 2, z: 4, core: 2. Of those that a mesh axis runs over, the one named last changes fastest.
Arguments:
- start_value: float32 [64, 32, 2048], P('sector', None, 'cap'), may hold values from 0 to 4
- firm_mass: float32 [64, 32, 2048], P('sector', None, 'cap'), may hold values from 0.1 to 10
- survive: int32 [64, 32, 2048], P('sector', None, 'cap'), may hold values from 0 to 1, as said below
- exit_index: int32 [64], P('sector'), may hold values from 0 to 8
- demand: float32 [64], P('sector'), may hold values from 0.3 to 90, as said below
- transition: float32 [32, 32], replicated, may hold values from 0 to 1, as said below
- install_cost: float32 [2048], P('cap'), may hold values from 0 to 1
Outputs:
- final_value: float32 [64, 32, 2048], P('sector', None, 'cap')
- rel_prices: float32 [64], P('sector')
The draws below stay inside these ranges and needn't reach their ends.
Inputs may be any that keep to these rules, and one draw needn't show every extreme that they name: `survive`: 0 or 1; the share of ones differs from sector to sector, from about a tenth to all. `demand`: positive, rising over the sectors by some thirty times. `transition`: entries positive, every row sums to one.
All inputs are finite; a program needn't handle non-finite values.
Results may differ from the reference program's by a relative error of at most 0.0003.
Values sent between devices are 32-bit elements; how exact they have to be, the bound alone decides.
A program may use at most 64 MiB of HBM per device.

```python
import math
import jax
import jax.numpy as jnp
from jax import lax

K = 2048
Z = 32
SWEEPS = 2
S = 64


def draw_survive(key, part):
    first_key, second_key = jax.random.split(jax.random.fold_in(key, 11))
    shares = jax.random.randint(first_key, (S, 1, 1), 10, 101)
    rolled = jax.random.randint(second_key, (S, Z, K), 0, 100)
    return (rolled < shares).astype(jnp.int32)


def draw_demand(key, part):
    sector_pos = jnp.arange(S).astype(jnp.float32)
    base = jnp.exp(jnp.log(30.0) * sector_pos / max(S - 1, 1))
    noise = jax.random.uniform(jax.random.fold_in(key, 21), (S,), minval=-0.5, maxval=0.5)
    return (base * jnp.exp(noise)).astype(jnp.float32)


def draw_transition(key, part):
    states = jnp.arange(Z)
    spread = jnp.abs(states[:, None] - states[None, :]).astype(jnp.float32)
    raw = jax.random.uniform(jax.random.fold_in(key, 31), (Z, Z), minval=0.3, maxval=1.0) * jnp.exp(-spread / 4.0)
    raw = raw + jnp.eye(Z, dtype=jnp.float32)
    return (raw / jnp.sum(raw, axis=1, keepdims=True)).astype(jnp.float32)


def touch_ends(values, own_key, smallest, top_value):
    shape = values.shape
    spot = [jax.random.randint(jax.random.fold_in(own_key, axis), (), 0, shape[axis]) for axis in range(len(shape))]
    values = values.at[tuple(spot)].set(smallest)
    longest = shape.index(max(shape))
    spot[longest] = (spot[longest] + 1) % shape[longest]
    return values.at[tuple(spot)].set(top_value)


def levels(own_key, dims, cuts, least, high):
    loudness, own = 1.0, jax.random.fold_in(own_key, 6)
    for position, blocks in cuts:
        steps = jnp.exp(jax.random.uniform(jax.random.fold_in(own, position), (blocks,), jnp.float32, least / len(cuts), high / len(cuts)))
        loudness = loudness * jnp.repeat(steps, dims[position] // blocks).reshape([-1 if axis == position else 1 for axis in range(len(dims))])
    return loudness


def setup_inputs(seed: int = 0) -> dict:
    arg_keys = jax.random.split(jax.random.key(seed), 8)
    start_value = jnp.clip(4.0 * jax.random.uniform(arg_keys[0], (S, Z, K), jnp.float32) ** levels(arg_keys[0], (S, Z, K), ((0, 8), (2, 4)), -0.2, 0.2), 0.0, 4.0)
    firm_mass = jnp.clip(jnp.exp(math.log(10.0) - 4.6051702 * jax.random.uniform(arg_keys[1], (S, Z, K), jnp.float32) ** levels(arg_keys[1], (S, Z, K), ((0, 8), (2, 4)), -0.2, 0.2)), 0.1, 10.0)
    survive = draw_survive(jax.random.fold_in(arg_keys[7], 71), 0)
    exit_index = touch_ends(jax.random.randint(arg_keys[3], (S,), 0, Z // 4 + 1), jax.random.fold_in(arg_keys[3], 1), 0, (Z // 4 + 1) - 1).astype(jnp.int32)
    demand = draw_demand(jax.random.fold_in(arg_keys[7], 71), 0)
    transition = draw_transition(jax.random.fold_in(arg_keys[7], 71), 0)
    install_cost = jnp.clip(1.0 * jax.random.uniform(arg_keys[6], (K,), jnp.float32) ** levels(arg_keys[6], (K,), ((0, 4),), -0.2, 0.2), 0.0, 1.0)
    return dict(start_value=start_value, firm_mass=firm_mass, survive=survive, exit_index=exit_index, demand=demand, transition=transition, install_cost=install_cost)


def capital_of(positions):
    return 0.2 * jnp.exp(jnp.log(10.0) * positions.astype(jnp.float32) / (K - 1))

def charge_of(cap_now, cap_next, row_ids, col_ids):
    invest = cap_next - 0.9 * cap_now
    fixed = jnp.where(row_ids == col_ids, 0.0, 1.5 * cap_now)
    return invest + invest * invest / cap_now + fixed

def sector_best(forward_value):
    row_block = math.gcd(K, 256)
    col_ids = jnp.arange(K, dtype=jnp.int32)
    capital = capital_of(col_ids)

    def row_step(first_row):
        row_ids = first_row + jnp.arange(row_block, dtype=jnp.int32)
        rows = capital_of(row_ids)
        charge = charge_of(rows[:, None], capital[None, :], row_ids[:, None], col_ids[None, :])
        return lax.optimization_barrier(jnp.max(forward_value[:, None, :] - charge[None], axis=2))
    starts = (jnp.arange(K // row_block) * row_block).astype(jnp.int32)
    blocks = lax.map(row_step, starts)
    return blocks.transpose(1, 0, 2).reshape(Z, K)

def reference(start_value, firm_mass, survive, exit_index, demand, transition, install_cost):
    prod_index = jnp.arange(Z, dtype=jnp.int32)
    capital = capital_of(jnp.arange(K, dtype=jnp.int32))
    log_prod = -0.5 + prod_index.astype(jnp.float32) / (Z - 1)
    output = jnp.exp(log_prod)[:, None] * capital[None, :] ** 0.6
    scrap = 0.3 * capital
    live = (survive == 1) & (prod_index[None, :, None] >= exit_index[:, None, None])
    values = start_value
    relative = jnp.zeros((S,), jnp.float32)
    for sweep in range(SWEEPS):
        staying = jnp.where(live, jax.nn.sigmoid((values - scrap) / 0.5), 0.0)
        supply = 1.0 + lax.optimization_barrier(jnp.sum(firm_mass * staying * output, axis=(1, 2))) / (Z * K)
        prices = jnp.sqrt(demand / supply)
        price_index = jnp.mean(jnp.sqrt(prices)) ** 2
        relative = prices / price_index
        continuation = jnp.where(live, jnp.maximum(values, scrap), scrap)
        expect = jnp.einsum('zw,swk->szk', transition, continuation, precision=lax.Precision.HIGHEST)
        forward_value = 0.9 * expect - install_cost[None, None, :]
        best = lax.map(sector_best, forward_value)
        values = jnp.where(live, relative[:, None, None] * output + best, scrap)
    return (values, relative)
```

```python
import functools
import math

import jax
import jax.numpy as jnp
from jax import lax
from jax.experimental import pallas as pl
from jax.experimental.pallas import tpu as pltpu
from jax.sharding import PartitionSpec as P

SWEEPS = 2
CHUNK_SLOTS = 8
SLOTS = 16
MERGED = 16
RANGES = 4
MERGED_RANGES = 2
NEG = -1e30
LOG_TEN = math.log(10.0)


def capital_of(positions, total):
    return 0.2 * jnp.exp(LOG_TEN * positions.astype(jnp.float32) / (total - 1))


def charge_of(cap_now, cap_next, row_ids, col_ids):
    invest = cap_next - 0.9 * cap_now
    fixed = jnp.where(row_ids == col_ids, 0.0, 1.5 * cap_now)
    return invest + invest * invest / cap_now + fixed


def best_reply(forward_rows, row_first, row_count):
    total_rows, total_cols = forward_rows.shape
    cap_of = functools.partial(capital_of, total=total_cols)
    col_block = math.gcd(total_cols, 2048)
    row_block = math.gcd(row_count, 512)
    grp_limit = max(1, (1 << 24) // (row_block * col_block))
    grp_size = math.gcd(total_rows, 1 << min(total_rows, grp_limit).bit_length() - 1)
    groups = forward_rows.reshape(total_rows // grp_size, grp_size, total_cols)

    def one_group(group):
        row_ids = row_first + jnp.arange(row_count, dtype=jnp.int32)
        cap_rows = cap_of(row_ids)
        col_ids = jnp.arange(total_cols, dtype=jnp.int32)
        cap_cols = cap_of(col_ids)
        charge = charge_of(cap_rows[:, None], cap_cols[None, :], row_ids[:, None], col_ids[None, :])
        return jnp.max(group[:, None, :] - charge[None], axis=2)

    return lax.map(one_group, groups).reshape(total_rows, row_count)


def gather_blocks(block, axis_name):
    count = lax.axis_size(axis_name)
    me = lax.axis_index(axis_name)
    parts = [block]
    for off in range(1, count):
        parts.append(lax.ppermute(block, axis_name, [(d, (d + off) % count) for d in range(count)]))
    return jnp.take(jnp.stack(parts), (me - jnp.arange(count) + count) % count, axis=0)


def dense_sweeps(start_value, firm_mass, survive, exit_index, demand, transition, install_cost):
    sec_dev, prod_count, cap_dev = start_value.shape
    sectors_all = sec_dev * lax.axis_size("sector")
    row_first = lax.axis_index("cap") * cap_dev
    prod_index = jnp.arange(prod_count, dtype=jnp.int32)
    total = cap_dev * lax.axis_size("cap")
    capital = capital_of(row_first + jnp.arange(cap_dev, dtype=jnp.int32), total)
    log_prod = -0.5 + prod_index.astype(jnp.float32) / (prod_count - 1)
    output = jnp.exp(log_prod)[:, None] * capital[None, :] ** 0.6
    scrap = 0.3 * capital
    live = (survive == 1) & (prod_index[None, :, None] >= exit_index[:, None, None])
    values = start_value
    relative = jnp.zeros((sec_dev,), jnp.float32)
    for sweep in range(SWEEPS):
        staying = jnp.where(live, jax.nn.sigmoid((values - scrap) / 0.5), 0.0)
        partial_value = jnp.sum(firm_mass * staying * output, axis=(1, 2))
        supply = 1.0 + jnp.sum(gather_blocks(partial_value, "cap"), axis=0) / (prod_count * total)
        prices = jnp.sqrt(demand / supply)
        root_sum = jnp.sum(gather_blocks(jnp.sqrt(prices), "sector"))
        price_index = (root_sum / sectors_all) ** 2
        relative = prices / price_index
        continuation = jnp.where(live, jnp.maximum(values, scrap), scrap)
        expect = jnp.einsum(
            "zw,swk->szk", transition, continuation, precision=lax.Precision.HIGHEST
        )
        forward_value = 0.9 * expect - install_cost[None, None, :]
        blocks = gather_blocks(forward_value, "cap")
        rows = jnp.moveaxis(blocks, 0, 2).reshape(sec_dev * prod_count, total)
        best = best_reply(rows, row_first, cap_dev).reshape(sec_dev, prod_count, cap_dev)
        values = jnp.where(live, relative[:, None, None] * output + best, scrap)
    return (values, relative)


def rows_of(step):
    return pl.ds(pl.multiple_of(step * 8, 8), 8)


def all_max(parts):
    return functools.reduce(jnp.maximum, parts)


def bases(tot_ref, count, sub, first, last):
    before, after = [], []
    for e in range(count):
        rows = [tot_ref[e, a:a + 1, :] for a in range(8)]
        if e < count - 1:
            before.append(all_max([jnp.where(sub > a, rows[a], NEG) for a in range(7)]))
        if e > 0:
            after.append(all_max([jnp.where(sub < a, rows[a], NEG) for a in range(1, 8)]))
    return before, after


def counts_before(tot_ref, counts, sub):
    tot_ref[0] = counts
    base = jnp.zeros_like(counts)
    for a in range(7):
        base = base + jnp.where(sub > a, tot_ref[0, a:a + 1, :], 0.0)
    return base


def useful(points, runs, sufs, afters):
    keep = None
    for e in range(len(runs)):
        good = (points[e] > runs[e]) & (points[e + 1] > jnp.maximum(sufs[e], afters[e]))
        keep = good if keep is None else keep | good
    return keep


def sweeps_kernel(n_sec, n_cap, start_hbm, mass_hbm, survive_hbm, exit_hbm, demand_hbm, trans_hbm, cost_hbm,
                  out_ref, cand_ref, rel_ref, flag_ref,
                  start_v, mass_v, survive_v, exit_v, demand_v, trans_v, cost_v,
                  nat_ref, val_ref, live_ref, g_ref, suf_ref, best_ref, col_ref, qt_ref,
                  weight_ref, ones_ref, tot_ref, l1_ref, pick_ref, zsum_ref, price_ref,
                  msg_ref, gat_ref, dem_ref, dems_ref, flg_ref, flgs_ref, pay_ref, pays_ref, size_ref,
                  in_sem, msg_send, msg_recv, dem_send, dem_recv, flg_send, flg_recv, pay_send, pay_recv):
    sec_dev, prods, cap_dev = start_v.shape
    total = cap_dev * n_cap
    steps = cap_dev // 8
    tiles = sec_dev * prods // 128
    tile_sec = 128 // prods
    lanes = tiles * 128
    col_tiles = cap_dev // 128
    n_dev = n_sec * n_cap
    me_cap = lax.axis_index("cap")
    me_sec = lax.axis_index("sector")
    me = me_sec * n_cap + me_cap
    my_row = me_cap * n_sec + me_sec
    mesh_id = pl.DeviceIdType.MESH
    f32 = jnp.float32

    def device(index):
        return {"sector": index // n_cap, "cap": lax.rem(index, n_cap)}

    barrier = pltpu.get_barrier_semaphore()

    def greet(off, carry):
        pl.semaphore_signal(barrier, inc=1, device_id=device(lax.rem(me + off, n_dev)), device_id_type=mesh_id)
        return carry

    lax.fori_loop(1, n_dev, greet, 0)
    loads = []
    for at, (src, dst) in enumerate((
        (trans_hbm, trans_v), (cost_hbm, cost_v), (exit_hbm, exit_v), (demand_hbm, demand_v),
        (mass_hbm, mass_v), (survive_hbm, survive_v), (start_hbm, start_v),
    )):
        loads.append(pltpu.make_async_copy(src, dst, in_sem.at[at]))
        loads[-1].start()

    sub = lax.broadcasted_iota(jnp.int32, (8, 128), 0)
    subf = sub.astype(f32)
    lane = lax.broadcasted_iota(jnp.int32, (1, 128), 1)
    lane_prod = lax.rem(lane, prods)
    lane_sec = lane // prods
    ends = [0.5 * 10.0 ** (e / RANGES) for e in range(RANGES + 1)]
    ends[0] *= 1.0 - 1e-5
    ends[-1] *= 1.0 + 1e-5
    first = me_cap * cap_dev
    CAP, SLOPE, POW, GADD, SQUARE = range(5)

    row = lax.broadcasted_iota(jnp.int32, (cap_dev, 128), 0)
    place = first + lax.rem(row, 8) * steps + row // 8
    capital = capital_of(place, total)
    col_ref[CAP] = capital
    col_ref[SLOPE] = 1.0 / capital
    col_ref[POW] = jnp.exp(0.6 * (math.log(0.2) + LOG_TEN * place.astype(f32) / (total - 1)))
    col_ref[SQUARE] = capital * capital
    for e in range(RANGES + 1):
        qt_ref[e] = capital * capital * ends[e]
    edge = [first + cap_dev - 1, first]
    t_low, t_high = [1.0 / capital_of(jnp.full((8, 128), at, jnp.int32), total) for at in edge]
    t_low, t_high = t_low * (1.0 - 1e-5), t_high * (1.0 + 1e-5)
    log_low, log_high = jnp.log(t_low), jnp.log(t_high)
    near = [t_low] + [
        jnp.exp(log_low + (log_high - log_low) * (e / MERGED_RANGES)) for e in range(1, MERGED_RANGES)
    ] + [t_high]
    prod_row = jnp.exp(-0.5 + lane_prod.astype(f32) / (prods - 1))
    big_r = lax.broadcasted_iota(jnp.int32, (128, 128), 0)
    big_c = lax.broadcasted_iota(jnp.int32, (128, 128), 1)
    same = big_r // prods == big_c // prods
    ones_ref[...] = jnp.where(same, 1.0, 0.0)

    loads[0].wait()
    spot_r = lax.broadcasted_iota(jnp.int32, (128, prods), 0)
    spot_c = lax.broadcasted_iota(jnp.int32, (128, prods), 1)
    spot = jnp.where(lax.rem(spot_r, prods) == spot_c, 1.0, 0.0)
    dims = (((1,), (1,)), ((), ()))
    half = lax.dot_general(spot, trans_v[...], dims, precision=lax.Precision.HIGHEST, preferred_element_type=f32)
    full = lax.dot_general(half, spot, dims, precision=lax.Precision.HIGHEST, preferred_element_type=f32)
    weight = jnp.where(same, 0.9 * full, 0.0)
    top = weight.astype(jnp.bfloat16)
    low = (weight - top.astype(f32)).astype(jnp.bfloat16)
    weight_ref[0:128, 0:128] = top
    weight_ref[128:256, 0:128] = top
    weight_ref[0:128, 128:256] = low
    weight_ref[128:256, 128:256] = jnp.zeros_like(low)

    loads[1].wait()
    for at in range(0, cap_dev, 128):
        nat_ref[0, at:at + 128, :] = jnp.broadcast_to(cost_v[:, at:at + 128], (128, 128)).T

    def add_step(i, carry):
        rows = rows_of(i)
        col_ref[GADD, rows, :] = 0.8 * col_ref[CAP, rows, :] - nat_ref[0, pl.ds(i, 8, stride=steps), :]
        return carry

    lax.fori_loop(0, steps, add_step, 0, unroll=4)

    loads[2].wait()
    loads[3].wait()
    exit_rows, demand_rows = [], []
    for t in range(tiles):
        exit_row = jnp.zeros((1, 128), jnp.int32)
        demand_row = jnp.zeros((1, 128), f32)
        for s in range(tile_sec):
            exit_row = jnp.where(lane_sec == s, exit_v[t * tile_sec + s], exit_row)
            demand_row = jnp.where(lane_sec == s, demand_v[t * tile_sec + s], demand_row)
        exit_rows.append(lane_prod >= exit_row)
        demand_rows.append(demand_row)
    dem_ref[...] = jnp.concatenate(demand_rows, axis=1)

    loads[4].wait()
    loads[5].wait()
    for t in range(tiles):
        secs = slice(t * tile_sec, (t + 1) * tile_sec)
        for at in range(0, cap_dev, 128):
            block = jnp.where(survive_v[secs, :, at:at + 128] == 1, mass_v[secs, :, at:at + 128], 0.0)
            nat_ref[t, at:at + 128, :] = block.reshape(128, 128).T

    for t in range(tiles):
        def live_step(i, carry, t=t):
            live_ref[t, rows_of(i), :] = jnp.where(exit_rows[t], nat_ref[t, pl.ds(i, 8, stride=steps), :], 0.0)
            return carry

        lax.fori_loop(0, steps, live_step, 0, unroll=4)
    loads[6].wait()
    for t in range(tiles):
        secs = slice(t * tile_sec, (t + 1) * tile_sec)
        for at in range(0, cap_dev, 128):
            nat_ref[t, at:at + 128, :] = start_v[secs, :, at:at + 128].reshape(128, 128).T

    def weigh(t, rows, value):
        scrap = 0.3 * col_ref[CAP, rows, :]
        stay = 1.0 / (1.0 + jnp.exp(2.0 * (scrap - value)))
        return live_ref[t, rows, :] * stay * col_ref[POW, rows, :]

    def send_supply(sweep, sums):
        grouped = jnp.dot(
            jnp.concatenate([part * prod_row for part in sums], axis=0), ones_ref[...],
            precision=lax.Precision.HIGHEST, preferred_element_type=f32)
        zsum_ref[...] = grouped
        for t in range(tiles):
            line = zsum_ref[t * 8:t * 8 + 1, :]
            for a in range(1, 8):
                line = line + zsum_ref[t * 8 + a:t * 8 + a + 1, :]
            msg_ref[sweep, :, t * 128:(t + 1) * 128] = line

        def post(off, carry):
            message(sweep, off).start()
            return carry

        lax.fori_loop(1, n_dev, post, 0)
        gat_ref[sweep, pl.ds(my_row, 1), :] = msg_ref[sweep]

    def message(sweep, off):
        return pltpu.make_async_remote_copy(
            src_ref=msg_ref.at[sweep], dst_ref=gat_ref.at[sweep, pl.ds(my_row, 1), :],
            send_sem=msg_send.at[sweep], recv_sem=msg_recv.at[sweep],
            device_id=device(lax.rem(me + off, n_dev)), device_id_type=mesh_id)

    def wait_rows(count, width, sem):
        view = size_ref.at[pl.ds(0, count), :, pl.ds(0, width)]
        pltpu.make_async_copy(view, view, sem).wait()

    def prices_row(sweep):
        wait_rows(n_dev - 1, lanes + 128, msg_recv.at[sweep])
        every = gat_ref[sweep, 0:n_sec, 0:lanes]
        for c in range(1, n_cap):
            every = every + gat_ref[sweep, c * n_sec:(c + 1) * n_sec, 0:lanes]
        supply = 1.0 + every / (prods * total)
        prices = jnp.sqrt(dems_ref[...] / supply)
        price_ref[...] = prices
        mean = jnp.sum(jnp.sqrt(prices), keepdims=True) / (lanes * n_sec)
        return price_ref[pl.ds(me_sec, 1), :] / (mean * mean)

    def forward(t):
        def chunk(at, carry):
            rows = pl.ds(pl.multiple_of(at * 128, 128), 128)
            cont = jnp.maximum(val_ref[t, rows, :], 0.3 * col_ref[CAP, rows, :])
            upper = cont.astype(jnp.bfloat16)
            lower = (cont - upper.astype(f32)).astype(jnp.bfloat16)
            both = jnp.dot(jnp.concatenate([upper, lower], axis=1), weight_ref[...], preferred_element_type=f32)
            g_ref[t, rows, :] = both[:, 0:128] + both[:, 128:256] + col_ref[GADD, rows, :]
            return carry

        lax.fori_loop(0, col_tiles, chunk, 0)

    def collect(rows_list, rank_rows, count):
        picks = [jnp.full((8, 128), NEG, f32) for _ in range(count // 8)]
        squares = [jnp.zeros((8, 128), f32) for _ in range(count // 8)]
        for (gain, square), rank in zip(rows_list, rank_rows):
            for h in range(count // 8):
                here = rank == subf + 8.0 * h
                picks[h] = jnp.where(here, gain, picks[h])
                squares[h] = jnp.where(here, square, squares[h])
        return picks, squares

    def prune(sweep, t):
        def back(at, runs):
            i = steps - 1 - at
            rows = rows_of(i)
            gain = g_ref[t, rows, :]
            points = [gain - qt_ref[e, rows, :] for e in range(RANGES + 1)]
            for e in range(RANGES):
                suf_ref[e, rows, :] = runs[e + 1]
            return tuple(jnp.maximum(run, point) for run, point in zip(runs, points))

        runs = lax.fori_loop(0, steps, back, (jnp.full((8, 128), NEG, f32),) * (RANGES + 1), unroll=4)
        for e in range(RANGES + 1):
            tot_ref[e] = runs[e]
        before, after = bases(tot_ref, RANGES + 1, sub, 0, 7)

        def ahead(i, carry):
            runs, counts, gains, squares = carry
            rows = rows_of(i)
            gain = g_ref[t, rows, :]
            square = col_ref[SQUARE, rows, :]
            points = [gain - qt_ref[e, rows, :] for e in range(RANGES + 1)]
            keep = useful(points, runs, [suf_ref[e, rows, :] for e in range(RANGES)], after)
            runs = tuple(jnp.maximum(run, point) for run, point in zip(runs, points))
            gains = tuple(jnp.where(keep, new, old) for new, old in zip((gain,) + gains, gains))
            squares = tuple(jnp.where(keep, new, old) for new, old in zip((square,) + squares, squares))
            return runs, counts + jnp.where(keep, 1.0, 0.0), gains, squares

        zero = jnp.zeros((8, 128), f32)
        runs, counts, gains, squares = lax.fori_loop(
            0, steps, ahead, (tuple(before), zero, (zero,) * CHUNK_SLOTS, (zero,) * CHUNK_SLOTS), unroll=4)
        base = counts_before(tot_ref, counts, sub)
        for p in range(CHUNK_SLOTS):
            l1_ref[0, p * 8:(p + 1) * 8, :] = gains[p]
            l1_ref[1, p * 8:(p + 1) * 8, :] = squares[p]
            l1_ref[2, p * 8:(p + 1) * 8, :] = jnp.where(counts > p, base + counts - (p + 1.0), -1.0)
        spots = range(CHUNK_SLOTS * 8)
        picks, squares = collect(
            [(l1_ref[0, r:r + 1, :], l1_ref[1, r:r + 1, :]) for r in spots],
            [l1_ref[2, r:r + 1, :] for r in spots], SLOTS)
        mine = pl.ds(pl.multiple_of(me_cap * SLOTS, SLOTS), SLOTS)
        for h in range(SLOTS // 8):
            pay_ref[sweep, t, 0, h * 8:(h + 1) * 8, :] = picks[h]
            pay_ref[sweep, t, 1, h * 8:(h + 1) * 8, :] = squares[h]
        for off in range(1, n_cap):
            payment(sweep, t, off).start()
        pays_ref[sweep, t, :, mine, :] = pay_ref[sweep, t]
        return jnp.where((counts > CHUNK_SLOTS) | (base + counts > SLOTS), 1.0, 0.0)

    def payment(sweep, t, off):
        mine = pl.ds(pl.multiple_of(me_cap * SLOTS, SLOTS), SLOTS)
        return pltpu.make_async_remote_copy(
            src_ref=pay_ref.at[sweep, t], dst_ref=pays_ref.at[sweep, t, :, mine, :],
            send_sem=pay_send.at[sweep, t], recv_sem=pay_recv.at[sweep, t],
            device_id={"cap": lax.rem(me_cap + off, n_cap)}, device_id_type=mesh_id)

    def pay_view(sweep, t):
        return pays_ref.at[sweep, t, :, pl.ds(0, (n_cap - 1) * SLOTS), :]

    def merge(sweep, t):
        pltpu.make_async_copy(pay_view(sweep, t), pay_view(sweep, t), pay_recv.at[sweep, t]).wait()
        hops = n_cap * SLOTS // 8

        def line(i):
            spots = pl.ds(i, 8, stride=hops)
            return pays_ref[sweep, t, 0, spots, :], pays_ref[sweep, t, 1, spots, :]

        def back(at, runs):
            i = hops - 1 - at
            gain, square = line(i)
            points = [gain - square * near[e] for e in range(MERGED_RANGES + 1)]
            for e in range(MERGED_RANGES):
                suf_ref[e, rows_of(i), :] = runs[e + 1]
            return tuple(jnp.maximum(run, point) for run, point in zip(runs, points))

        runs = lax.fori_loop(0, hops, back, (jnp.full((8, 128), NEG, f32),) * (MERGED_RANGES + 1), unroll=8)
        for e in range(MERGED_RANGES + 1):
            tot_ref[e] = runs[e]
        before, after = bases(tot_ref, MERGED_RANGES + 1, sub, 0, 7)

        def ahead(i, carry):
            runs, counts = carry
            gain, square = line(i)
            points = [gain - square * near[e] for e in range(MERGED_RANGES + 1)]
            keep = useful(points, runs, [suf_ref[e, rows_of(i), :] for e in range(MERGED_RANGES)], after)
            runs = tuple(jnp.maximum(run, point) for run, point in zip(runs, points))
            pick_ref[0, rows_of(i), :] = jnp.where(keep, counts, NEG)
            return runs, counts + jnp.where(keep, 1.0, 0.0)

        runs, counts = lax.fori_loop(0, hops, ahead, (tuple(before), jnp.zeros((8, 128), f32)), unroll=8)
        base = counts_before(tot_ref, counts, sub)
        for i in range(hops):
            pick_ref[0, i * 8:(i + 1) * 8, :] = pick_ref[0, i * 8:(i + 1) * 8, :] + base
        spots = [(i, a) for i in range(hops) for a in range(8)]
        picks, squares = collect(
            [(pays_ref[sweep, t, 0, a * hops + i:a * hops + i + 1, :],
              pays_ref[sweep, t, 1, a * hops + i:a * hops + i + 1, :]) for i, a in spots],
            [pick_ref[0, i * 8 + a:i * 8 + a + 1, :] for i, a in spots], MERGED)
        for h in range(MERGED // 8):
            pick_ref[1, h * 8:(h + 1) * 8, :] = picks[h]
            pick_ref[2, h * 8:(h + 1) * 8, :] = squares[h]
        return jnp.where(base + counts > MERGED, 1.0, 0.0)

    def reply(t):
        gains = [jnp.broadcast_to(pick_ref[1, c:c + 1, :], (8, 128)) for c in range(MERGED)]
        squares = [jnp.broadcast_to(pick_ref[2, c:c + 1, :], (8, 128)) for c in range(MERGED)]

        def one(i, carry):
            rows = rows_of(i)
            slope = col_ref[SLOPE, rows, :]
            capital = col_ref[CAP, rows, :]
            moved = all_max([gain - square * slope for gain, square in zip(gains, squares)])
            best_ref[t, rows, :] = jnp.maximum(moved - 1.41 * capital, g_ref[t, rows, :] - 0.91 * capital)
            return carry

        lax.fori_loop(0, steps, one, 0, unroll=4)

    sums = []
    for t in range(tiles):
        def open_step(i, acc, t=t):
            rows = rows_of(i)
            value = jnp.where(live_ref[t, rows, :] > 0.0, nat_ref[t, pl.ds(i, 8, stride=steps), :],
                              0.3 * col_ref[CAP, rows, :])
            val_ref[t, rows, :] = value
            return acc + weigh(t, rows, value)

        sums.append(lax.fori_loop(0, steps, open_step, jnp.zeros((8, 128), f32), unroll=8))
    pl.semaphore_wait(barrier, n_dev - 1)
    dem_copies = []
    for off in range(1, n_sec):
        dem_copies.append(pltpu.make_async_remote_copy(
            src_ref=dem_ref, dst_ref=dems_ref.at[pl.ds(me_sec, 1), :], send_sem=dem_send, recv_sem=dem_recv,
            device_id={"sector": lax.rem(me_sec + off, n_sec)}, device_id_type=mesh_id))
        dem_copies[-1].start()
    dems_ref[pl.ds(me_sec, 1), :] = dem_ref[...]
    msg_ref[0, :, lanes:lanes + 128] = jnp.zeros((1, 128), f32)

    def flag_row(flags):
        tot_ref[0] = flags
        return all_max([tot_ref[0, a:a + 1, :] for a in range(8)])

    late = None
    for sweep in range(SWEEPS):
        send_supply(sweep, sums)
        flags = jnp.zeros((8, 128), f32)
        for t in range(tiles):
            forward(t)
            flags = jnp.maximum(flags, prune(sweep, t))
        if sweep == SWEEPS - 1:
            flg_ref[...] = flag_row(flags)

            def report(off, carry):
                pltpu.make_async_remote_copy(
                    src_ref=flg_ref, dst_ref=flgs_ref.at[pl.ds(my_row, 1), :], send_sem=flg_send, recv_sem=flg_recv,
                    device_id=device(lax.rem(me + off, n_dev)), device_id_type=mesh_id).start()
                return carry

            lax.fori_loop(1, n_dev, report, 0)
            flgs_ref[pl.ds(my_row, 1), :] = flg_ref[...]
        late = jnp.zeros((8, 128), f32)
        for t in range(tiles):
            late = jnp.maximum(late, merge(sweep, t))
            reply(t)
        if sweep == 0:
            msg_ref[1, :, lanes:lanes + 128] = flag_row(jnp.maximum(flags, late))
            wait_rows(n_sec - 1, lanes, dem_recv)
        relative = prices_row(sweep)
        if sweep == 0:
            sums = []
            for t in range(tiles):
                scale = relative[:, t * 128:(t + 1) * 128] * prod_row

                def next_step(i, acc, t=t, scale=scale):
                    rows = rows_of(i)
                    value = jnp.where(live_ref[t, rows, :] > 0.0,
                                      scale * col_ref[POW, rows, :] + best_ref[t, rows, :],
                                      0.3 * col_ref[CAP, rows, :])
                    val_ref[t, rows, :] = value
                    return acc + weigh(t, rows, value)

                sums.append(lax.fori_loop(0, steps, next_step, jnp.zeros((8, 128), f32), unroll=8))
    for s in range(sec_dev):
        rel_ref[s] = relative[0, s * prods]
    for t in range(tiles):
        scale = relative[:, t * 128:(t + 1) * 128] * prod_row

        def last_step(i, carry, t=t, scale=scale):
            rows = rows_of(i)
            nat_ref[t, pl.ds(i, 8, stride=steps), :] = jnp.where(
                live_ref[t, rows, :] > 0.0, scale * col_ref[POW, rows, :] + best_ref[t, rows, :],
                0.3 * col_ref[CAP, rows, :])
            return carry

        lax.fori_loop(0, steps, last_step, 0, unroll=8)
        secs = slice(t * tile_sec, (t + 1) * tile_sec)
        for at in range(0, cap_dev, 128):
            out_ref[secs, :, at:at + 128] = nat_ref[t, at:at + 128, :].T.reshape(tile_sec, prods, 128)
    cand_ref[...] = pays_ref[SWEEPS - 1]
    wait_rows(n_dev - 1, 128, flg_recv)
    bad = jnp.max(jnp.maximum(jnp.max(flgs_ref[...], axis=0, keepdims=True),
                              jnp.max(gat_ref[1, :, lanes:lanes + 128], axis=0, keepdims=True)))
    flag_ref[0] = jnp.where(bad > 0.0, 2, jnp.where(jnp.max(late) > 0.0, 1, 0)).astype(jnp.int32)

    for sweep in range(SWEEPS):
        wait_rows(n_dev - 1, lanes + 128, msg_send.at[sweep])
        for t in range(tiles):
            pltpu.make_async_copy(pay_view(sweep, t), pay_view(sweep, t), pay_send.at[sweep, t]).wait()
    wait_rows(n_dev - 1, 128, flg_send)
    wait_rows(n_sec - 1, lanes, dem_send)


def pruned_sweeps(start_value, firm_mass, survive, exit_index, demand, transition, install_cost):
    n_sec, n_cap = lax.axis_size("sector"), lax.axis_size("cap")
    sec_dev, prods, cap_dev = start_value.shape
    lanes = sec_dev * prods
    tiles = lanes // 128
    n_dev = n_sec * n_cap
    far = pl.BlockSpec(memory_space=pl.ANY)
    vmem = pl.BlockSpec(memory_space=pltpu.VMEM)
    smem = pl.BlockSpec(memory_space=pltpu.SMEM)
    f32 = jnp.float32
    dma = pltpu.SemaphoreType.DMA
    pack = max(RANGES, MERGED_RANGES)
    return pl.pallas_call(
        functools.partial(sweeps_kernel, n_sec, n_cap),
        out_shape=(
            jax.ShapeDtypeStruct(start_value.shape, f32),
            jax.ShapeDtypeStruct((tiles, 2, n_cap * SLOTS, 128), f32),
            jax.ShapeDtypeStruct((sec_dev,), f32),
            jax.ShapeDtypeStruct((1,), jnp.int32),
        ),
        in_specs=[far] * 7,
        out_specs=(vmem, vmem, smem, smem),
        scratch_shapes=[
            pltpu.VMEM(start_value.shape, f32),
            pltpu.VMEM(start_value.shape, f32),
            pltpu.VMEM(start_value.shape, jnp.int32),
            pltpu.SMEM((sec_dev,), jnp.int32),
            pltpu.SMEM((sec_dev,), f32),
            pltpu.VMEM((prods, prods), f32),
            pltpu.VMEM((1, cap_dev), f32),
            pltpu.VMEM((tiles, cap_dev, 128), f32),
            pltpu.VMEM((tiles, cap_dev, 128), f32),
            pltpu.VMEM((tiles, cap_dev, 128), f32),
            pltpu.VMEM((tiles, cap_dev, 128), f32),
            pltpu.VMEM((pack, max(cap_dev, n_cap * SLOTS), 128), f32),
            pltpu.VMEM((tiles, cap_dev, 128), f32),
            pltpu.VMEM((5, cap_dev, 128), f32),
            pltpu.VMEM((RANGES + 1, cap_dev, 128), f32),
            pltpu.VMEM((256, 256), jnp.bfloat16),
            pltpu.VMEM((128, 128), f32),
            pltpu.VMEM((pack + 1, 8, 128), f32),
            pltpu.VMEM((3, CHUNK_SLOTS * 8, 128), f32),
            pltpu.VMEM((3, max(MERGED, n_cap * SLOTS), 128), f32),
            pltpu.VMEM((tiles * 8, 128), f32),
            pltpu.VMEM((n_sec, lanes), f32),
            pltpu.VMEM((SWEEPS, 1, lanes + 128), f32),
            pltpu.VMEM((SWEEPS, n_dev, lanes + 128), f32),
            pltpu.VMEM((1, lanes), f32),
            pltpu.VMEM((n_sec, lanes), f32),
            pltpu.VMEM((1, 128), f32),
            pltpu.VMEM((n_dev, 128), f32),
            pltpu.VMEM((SWEEPS, tiles, 2, SLOTS, 128), f32),
            pltpu.VMEM((SWEEPS, tiles, 2, n_cap * SLOTS, 128), f32),
            pltpu.VMEM((n_dev - 1, 1, lanes + 128), f32),
            dma((7,)),
            dma((SWEEPS,)), dma((SWEEPS,)), dma, dma, dma, dma,
            dma((SWEEPS, tiles)), dma((SWEEPS, tiles)),
        ],
        compiler_params=pltpu.CompilerParams(
            collective_id=0, has_side_effects=True, vmem_limit_bytes=48 * 1024 * 1024
        ),
    )(start_value, firm_mass, survive, exit_index, demand, transition, install_cost[None, :])


def all_candidates(values, candidates, relative, survive, exit_index):
    sec_dev, prods, cap_dev = values.shape
    total = cap_dev * lax.axis_size("cap")
    capital = capital_of(lax.axis_index("cap") * cap_dev + jnp.arange(cap_dev, dtype=jnp.int32), total)
    prod_index = jnp.arange(prods, dtype=jnp.int32)
    output = jnp.exp(-0.5 + prod_index.astype(jnp.float32) / (prods - 1))[:, None] * capital[None, :] ** 0.6
    live = (survive == 1) & (prod_index[None, :, None] >= exit_index[:, None, None])
    flat = jnp.moveaxis(candidates, 0, 2).reshape(2, candidates.shape[2], sec_dev, prods)

    def one(best, pair):
        return jnp.maximum(best, pair[0][:, :, None] - pair[1][:, :, None] / capital), None

    moved, _ = lax.scan(one, jnp.full(values.shape, NEG, jnp.float32), (flat[0], flat[1]))
    again = relative[:, None, None] * output + (moved - 1.41 * capital)
    return jnp.where(live, jnp.maximum(values, again), values)


def on_device(start_value, firm_mass, survive, exit_index, demand, transition, install_cost):
    args = (start_value, firm_mass, survive, exit_index, demand, transition, install_cost)
    sec_dev, prods, cap_dev = start_value.shape
    if 128 % prods or prods % 8 or sec_dev * prods % 128 or cap_dev % 128 or min(
            lax.axis_size("sector"), lax.axis_size("cap")) < 2:
        return dense_sweeps(*args)
    values, candidates, relative, state = pruned_sweeps(*args)
    return lax.switch(
        state[0],
        (
            lambda: (values, relative),
            lambda: (all_candidates(values, candidates, relative, survive, exit_index), relative),
            lambda: dense_sweeps(*args),
        ),
    )


def solution(mesh):
    return jax.shard_map(
        on_device,
        mesh=mesh,
        in_specs=(
            P("sector", None, "cap"),
            P("sector", None, "cap"),
            P("sector", None, "cap"),
            P("sector"),
            P("sector"),
            P(),
            P("cap"),
        ),
        out_specs=(P("sector", None, "cap"), P("sector")),
        check_vma=False,
    )
```

```python
import functools
import math

import jax
import jax.numpy as jnp
from jax import lax
from jax.experimental import pallas as pl
from jax.experimental.pallas import tpu as pltpu
from jax.sharding import PartitionSpec as P

SWEEPS = 2
CHUNK_SLOTS = 8
SLOTS = 16
MERGED = 12
UNROLLED_DEVICES = 64
RANGES = 4
MERGED_RANGES = 2
NEG = -1e30
LOG_TEN = math.log(10.0)


def capital_of(positions, total):
    return 0.2 * jnp.exp(LOG_TEN * positions.astype(jnp.float32) / (total - 1))


def charge_of(cap_now, cap_next, row_ids, col_ids):
    invest = cap_next - 0.9 * cap_now
    fixed = jnp.where(row_ids == col_ids, 0.0, 1.5 * cap_now)
    return invest + invest * invest / cap_now + fixed


def best_reply(forward_rows, row_first, row_count):
    total_rows, total_cols = forward_rows.shape
    cap_of = functools.partial(capital_of, total=total_cols)
    col_block = math.gcd(total_cols, 2048)
    row_block = math.gcd(row_count, 512)
    grp_limit = max(1, (1 << 24) // (row_block * col_block))
    grp_size = math.gcd(total_rows, 1 << min(total_rows, grp_limit).bit_length() - 1)
    groups = forward_rows.reshape(total_rows // grp_size, grp_size, total_cols)

    def one_group(group):
        row_ids = row_first + jnp.arange(row_count, dtype=jnp.int32)
        cap_rows = cap_of(row_ids)
        col_ids = jnp.arange(total_cols, dtype=jnp.int32)
        cap_cols = cap_of(col_ids)
        charge = charge_of(cap_rows[:, None], cap_cols[None, :], row_ids[:, None], col_ids[None, :])
        return jnp.max(group[:, None, :] - charge[None], axis=2)

    return lax.map(one_group, groups).reshape(total_rows, row_count)


def gather_blocks(block, axis_name):
    count = lax.axis_size(axis_name)
    me = lax.axis_index(axis_name)
    parts = [block]
    for off in range(1, count):
        parts.append(lax.ppermute(block, axis_name, [(d, (d + off) % count) for d in range(count)]))
    return jnp.take(jnp.stack(parts), (me - jnp.arange(count) + count) % count, axis=0)


def dense_sweeps(start_value, firm_mass, survive, exit_index, demand, transition, install_cost):
    sec_dev, prod_count, cap_dev = start_value.shape
    sectors_all = sec_dev * lax.axis_size("sector")
    row_first = lax.axis_index("cap") * cap_dev
    prod_index = jnp.arange(prod_count, dtype=jnp.int32)
    total = cap_dev * lax.axis_size("cap")
    capital = capital_of(row_first + jnp.arange(cap_dev, dtype=jnp.int32), total)
    log_prod = -0.5 + prod_index.astype(jnp.float32) / (prod_count - 1)
    output = jnp.exp(log_prod)[:, None] * capital[None, :] ** 0.6
    scrap = 0.3 * capital
    live = (survive == 1) & (prod_index[None, :, None] >= exit_index[:, None, None])
    values = start_value
    relative = jnp.zeros((sec_dev,), jnp.float32)
    for sweep in range(SWEEPS):
        staying = jnp.where(live, jax.nn.sigmoid((values - scrap) / 0.5), 0.0)
        partial_value = jnp.sum(firm_mass * staying * output, axis=(1, 2))
        supply = 1.0 + jnp.sum(gather_blocks(partial_value, "cap"), axis=0) / (prod_count * total)
        prices = jnp.sqrt(demand / supply)
        root_sum = jnp.sum(gather_blocks(jnp.sqrt(prices), "sector"))
        price_index = (root_sum / sectors_all) ** 2
        relative = prices / price_index
        continuation = jnp.where(live, jnp.maximum(values, scrap), scrap)
        expect = jnp.einsum(
            "zw,swk->szk", transition, continuation, precision=lax.Precision.HIGHEST
        )
        forward_value = 0.9 * expect - install_cost[None, None, :]
        blocks = gather_blocks(forward_value, "cap")
        rows = jnp.moveaxis(blocks, 0, 2).reshape(sec_dev * prod_count, total)
        best = best_reply(rows, row_first, cap_dev).reshape(sec_dev, prod_count, cap_dev)
        values = jnp.where(live, relative[:, None, None] * output + best, scrap)
    return (values, relative)


def rows_of(step):
    return pl.ds(pl.multiple_of(step * 8, 8), 8)


def all_max(parts):
    return functools.reduce(jnp.maximum, parts)


def bases(tot_ref, count, sub, first, last):
    before, after = [], []
    for e in range(count):
        rows = [tot_ref[e, a:a + 1, :] for a in range(8)]
        if e < count - 1:
            before.append(all_max([jnp.where(sub > a, rows[a], NEG) for a in range(7)]))
        if e > 0:
            after.append(all_max([jnp.where(sub < a, rows[a], NEG) for a in range(1, 8)]))
    return before, after


def counts_before(tot_ref, counts, sub):
    tot_ref[0] = counts
    base = jnp.zeros_like(counts)
    for a in range(7):
        base = base + jnp.where(sub > a, tot_ref[0, a:a + 1, :], 0.0)
    return base


def useful(points, runs, sufs, afters):
    keep = None
    for e in range(len(runs)):
        good = (points[e] > runs[e]) & (points[e + 1] > jnp.maximum(sufs[e], afters[e]))
        keep = good if keep is None else keep | good
    return keep


def sweeps_kernel(n_sec, n_cap, start_hbm, mass_hbm, survive_hbm, exit_hbm, demand_hbm, trans_hbm, cost_hbm,
                  out_ref, cand_ref, rel_ref, flag_ref,
                  start_v, mass_v, survive_v, exit_v, demand_v, trans_v, cost_v,
                  nat_ref, fresh_ref, val_ref, live_ref, g_ref, suf_ref, best_ref, col_ref, qt_ref,
                  weight_ref, ones_ref, tot_ref, l1_ref, pick_ref, zsum_ref, price_ref,
                  msg_ref, gat_ref, dem_ref, dems_ref, flg_ref, flgs_ref, pay_ref, pays_ref, size_ref,
                  in_sem, msg_send, msg_recv, dem_send, dem_recv, flg_send, flg_recv, pay_send, pay_recv):
    sec_dev, prods, cap_dev = start_v.shape
    total = cap_dev * n_cap
    steps = cap_dev // 8
    tiles = sec_dev * prods // 128
    tile_sec = 128 // prods
    lanes = tiles * 128
    col_tiles = cap_dev // 128
    n_dev = n_sec * n_cap
    me_cap = lax.axis_index("cap")
    me_sec = lax.axis_index("sector")
    me = me_sec * n_cap + me_cap
    my_row = me_cap * n_sec + me_sec
    mesh_id = pl.DeviceIdType.MESH
    f32 = jnp.float32

    def each_other(act):
        if n_dev > UNROLLED_DEVICES:
            def one(off, carry):
                index = lax.rem(me + off, n_dev)
                act({"sector": index // n_cap, "cap": lax.rem(index, n_cap)})
                return carry

            lax.fori_loop(1, n_dev, one, 0)
            return
        upper = me_sec * 2 // n_sec
        skip = me_sec + upper * (n_sec - 1 - 2 * me_sec)
        for j in range(n_sec - 1):
            spot = n_sec - 1 - j - (j + 1 + skip) // n_sec
            other = spot + upper * (n_sec - 1 - 2 * spot)
            for c in range(n_cap):
                act({"sector": other, "cap": lax.rem(me_cap + c, n_cap)})
        for c in range(1, n_cap):
            act({"sector": me_sec, "cap": lax.rem(me_cap + c, n_cap)})

    barrier = pltpu.get_barrier_semaphore()
    each_other(lambda device: pl.semaphore_signal(barrier, inc=1, device_id=device, device_id_type=mesh_id))
    loads = []
    for at, (src, dst) in enumerate((
        (trans_hbm, trans_v), (cost_hbm, cost_v), (exit_hbm, exit_v), (demand_hbm, demand_v),
        (mass_hbm, mass_v), (survive_hbm, survive_v), (start_hbm, start_v),
    )):
        loads.append(pltpu.make_async_copy(src, dst, in_sem.at[at]))
        loads[-1].start()

    sub = lax.broadcasted_iota(jnp.int32, (8, 128), 0)
    subf = sub.astype(f32)
    lane = lax.broadcasted_iota(jnp.int32, (1, 128), 1)
    lane_prod = lax.rem(lane, prods)
    lane_sec = lane // prods
    ends = [0.5 * 10.0 ** (e / RANGES) for e in range(RANGES + 1)]
    ends[0] *= 1.0 - 1e-5
    ends[-1] *= 1.0 + 1e-5
    first = me_cap * cap_dev
    CAP, SLOPE, POW, GADD, SQUARE = range(5)

    row = lax.broadcasted_iota(jnp.int32, (cap_dev, 128), 0)
    place = first + lax.rem(row, 8) * steps + row // 8
    capital = capital_of(place, total)
    col_ref[CAP] = capital
    col_ref[SLOPE] = 1.0 / capital
    col_ref[POW] = jnp.exp(0.6 * (math.log(0.2) + LOG_TEN * place.astype(f32) / (total - 1)))
    col_ref[SQUARE] = capital * capital
    for e in range(RANGES + 1):
        qt_ref[e] = capital * capital * ends[e]
    edge = [first + cap_dev - 1, first]
    t_low, t_high = [1.0 / capital_of(jnp.full((8, 128), at, jnp.int32), total) for at in edge]
    t_low, t_high = t_low * (1.0 - 1e-5), t_high * (1.0 + 1e-5)
    log_low, log_high = jnp.log(t_low), jnp.log(t_high)
    near = [t_low] + [
        jnp.exp(log_low + (log_high - log_low) * (e / MERGED_RANGES)) for e in range(1, MERGED_RANGES)
    ] + [t_high]
    prod_row = jnp.exp(-0.5 + lane_prod.astype(f32) / (prods - 1))
    big_r = lax.broadcasted_iota(jnp.int32, (128, 128), 0)
    big_c = lax.broadcasted_iota(jnp.int32, (128, 128), 1)
    same = big_r // prods == big_c // prods
    ones_ref[...] = jnp.where(same, 1.0, 0.0).astype(jnp.bfloat16)

    loads[0].wait()
    spot_r = lax.broadcasted_iota(jnp.int32, (128, prods), 0)
    spot_c = lax.broadcasted_iota(jnp.int32, (128, prods), 1)
    spot = jnp.where(lax.rem(spot_r, prods) == spot_c, 1.0, 0.0)
    dims = (((1,), (1,)), ((), ()))
    half = lax.dot_general(spot, trans_v[...], dims, precision=lax.Precision.HIGHEST, preferred_element_type=f32)
    full = lax.dot_general(half, spot, dims, precision=lax.Precision.HIGHEST, preferred_element_type=f32)
    weight = jnp.where(same, 0.9 * full, 0.0)
    top = weight.astype(jnp.bfloat16)
    low = (weight - top.astype(f32)).astype(jnp.bfloat16)
    weight_ref[0:128, 0:128] = top
    weight_ref[128:256, 0:128] = top
    weight_ref[0:128, 128:256] = low
    weight_ref[128:256, 128:256] = jnp.zeros_like(low)

    loads[1].wait()
    for at in range(0, cap_dev, 128):
        nat_ref[0, at:at + 128, :] = jnp.broadcast_to(cost_v[:, at:at + 128], (128, 128)).T

    def add_step(i, carry):
        rows = rows_of(i)
        col_ref[GADD, rows, :] = 0.8 * col_ref[CAP, rows, :] - nat_ref[0, pl.ds(i, 8, stride=steps), :]
        return carry

    lax.fori_loop(0, steps, add_step, 0, unroll=8)

    loads[2].wait()
    loads[3].wait()
    exit_rows, demand_rows = [], []
    for t in range(tiles):
        exit_row = jnp.zeros((1, 128), jnp.int32)
        demand_row = jnp.zeros((1, 128), f32)
        for s in range(tile_sec):
            exit_row = jnp.where(lane_sec == s, exit_v[t * tile_sec + s], exit_row)
            demand_row = jnp.where(lane_sec == s, demand_v[t * tile_sec + s], demand_row)
        exit_rows.append(lane_prod >= exit_row)
        demand_rows.append(demand_row)
    dem_ref[...] = jnp.concatenate(demand_rows, axis=1)

    loads[4].wait()
    loads[5].wait()
    for t in range(tiles):
        secs = slice(t * tile_sec, (t + 1) * tile_sec)
        for at in range(0, cap_dev, 128):
            block = jnp.where(survive_v[secs, :, at:at + 128] == 1, mass_v[secs, :, at:at + 128], 0.0)
            nat_ref[t, at:at + 128, :] = block.reshape(128, 128).T

    loads[6].wait()
    for t in range(tiles):
        secs = slice(t * tile_sec, (t + 1) * tile_sec)
        for at in range(0, cap_dev, 128):
            fresh_ref[t, at:at + 128, :] = start_v[secs, :, at:at + 128].reshape(128, 128).T

    def weigh(mass, rows, value):
        scrap = 0.3 * col_ref[CAP, rows, :]
        stay = 1.0 / (1.0 + jnp.exp(2.0 * (scrap - value)))
        return mass * stay * col_ref[POW, rows, :]

    def send_supply(sweep, sums):
        part = jnp.concatenate([one * prod_row for one in sums], axis=0)
        splits = []
        for _ in range(3):
            splits.append(part.astype(jnp.bfloat16).astype(f32))
            part = part - splits[-1]
        grouped = jnp.dot(jnp.concatenate(splits, axis=0).astype(jnp.bfloat16), ones_ref[...],
                          preferred_element_type=f32)
        zsum_ref[...] = grouped[0:tiles * 8] + grouped[tiles * 8:tiles * 16] + grouped[tiles * 16:]
        for t in range(tiles):
            line = zsum_ref[t * 8:t * 8 + 1, :]
            for a in range(1, 8):
                line = line + zsum_ref[t * 8 + a:t * 8 + a + 1, :]
            msg_ref[sweep, :, t * 128:(t + 1) * 128] = line

        each_other(lambda device: pltpu.make_async_remote_copy(
            src_ref=msg_ref.at[sweep], dst_ref=gat_ref.at[sweep, pl.ds(my_row, 1), :],
            send_sem=msg_send.at[sweep], recv_sem=msg_recv.at[sweep],
            device_id=device, device_id_type=mesh_id).start())
        gat_ref[sweep, pl.ds(my_row, 1), :] = msg_ref[sweep]

    def wait_rows(count, width, sem):
        view = size_ref.at[pl.ds(0, count), :, pl.ds(0, width)]
        pltpu.make_async_copy(view, view, sem).wait()

    def prices_row(sweep):
        wait_rows(n_dev - 1, lanes + 128, msg_recv.at[sweep])
        every = gat_ref[sweep, 0:n_sec, 0:lanes]
        for c in range(1, n_cap):
            every = every + gat_ref[sweep, c * n_sec:(c + 1) * n_sec, 0:lanes]
        supply = 1.0 + every / (prods * total)
        prices = jnp.sqrt(dems_ref[...] / supply)
        price_ref[...] = prices
        mean = jnp.sum(jnp.sqrt(prices), keepdims=True) / (lanes * n_sec)
        return price_ref[pl.ds(me_sec, 1), :] / (mean * mean)

    def forward(t):
        cont = jnp.maximum(val_ref[t], 0.3 * col_ref[CAP])
        upper = cont.astype(jnp.bfloat16)
        lower = (cont - upper.astype(f32)).astype(jnp.bfloat16)
        both = jnp.dot(jnp.concatenate([upper, lower], axis=1), weight_ref[...], preferred_element_type=f32)
        g_ref[t] = both[:, 0:128] + both[:, 128:256] + col_ref[GADD]

    def collect(rows_list, rank_rows, count):
        picks = [jnp.full((8, 128), NEG, f32) for _ in range(-(-count // 8))]
        squares = [jnp.zeros((8, 128), f32) for _ in range(-(-count // 8))]
        for (gain, square), rank in zip(rows_list, rank_rows):
            for h in range(-(-count // 8)):
                here = rank == subf + 8.0 * h
                picks[h] = jnp.where(here, gain, picks[h])
                squares[h] = jnp.where(here, square, squares[h])
        return picks, squares

    def prune(sweep, t):
        def back(at, runs):
            i = steps - 1 - at
            rows = rows_of(i)
            gain = g_ref[t, rows, :]
            points = [gain - qt_ref[e, rows, :] for e in range(RANGES + 1)]
            for e in range(RANGES):
                suf_ref[e, rows, :] = runs[e + 1]
            return tuple(jnp.maximum(run, point) for run, point in zip(runs, points))

        runs = lax.fori_loop(0, steps, back, (jnp.full((8, 128), NEG, f32),) * (RANGES + 1), unroll=16)
        for e in range(RANGES + 1):
            tot_ref[e] = runs[e]
        before, after = bases(tot_ref, RANGES + 1, sub, 0, 7)

        def ahead(i, carry):
            runs, counts, gains, squares = carry
            rows = rows_of(i)
            gain = g_ref[t, rows, :]
            square = col_ref[SQUARE, rows, :]
            points = [gain - qt_ref[e, rows, :] for e in range(RANGES + 1)]
            keep = useful(points, runs, [suf_ref[e, rows, :] for e in range(RANGES)], after)
            runs = tuple(jnp.maximum(run, point) for run, point in zip(runs, points))
            gains = tuple(jnp.where(keep, new, old) for new, old in zip((gain,) + gains, gains))
            squares = tuple(jnp.where(keep, new, old) for new, old in zip((square,) + squares, squares))
            return runs, counts + jnp.where(keep, 1.0, 0.0), gains, squares

        zero = jnp.zeros((8, 128), f32)
        runs, counts, gains, squares = lax.fori_loop(
            0, steps, ahead, (tuple(before), zero, (zero,) * CHUNK_SLOTS, (zero,) * CHUNK_SLOTS), unroll=8)
        base = counts_before(tot_ref, counts, sub)
        for p in range(CHUNK_SLOTS):
            l1_ref[0, p * 8:(p + 1) * 8, :] = gains[p]
            l1_ref[1, p * 8:(p + 1) * 8, :] = squares[p]
            l1_ref[2, p * 8:(p + 1) * 8, :] = jnp.where(counts > p, base + counts - (p + 1.0), -1.0)
        spots = range(CHUNK_SLOTS * 8)
        picks, squares = collect(
            [(l1_ref[0, r:r + 1, :], l1_ref[1, r:r + 1, :]) for r in spots],
            [l1_ref[2, r:r + 1, :] for r in spots], SLOTS)
        mine = pl.ds(pl.multiple_of(me_cap * SLOTS, SLOTS), SLOTS)
        for h in range(SLOTS // 8):
            pay_ref[sweep, t, 0, h * 8:(h + 1) * 8, :] = picks[h]
            pay_ref[sweep, t, 1, h * 8:(h + 1) * 8, :] = squares[h]
        for off in range(1, n_cap):
            payment(sweep, t, off).start()
        pays_ref[sweep, t, :, mine, :] = pay_ref[sweep, t]
        return jnp.where((counts > CHUNK_SLOTS) | (base + counts > SLOTS), 1.0, 0.0)

    def payment(sweep, t, off):
        mine = pl.ds(pl.multiple_of(me_cap * SLOTS, SLOTS), SLOTS)
        return pltpu.make_async_remote_copy(
            src_ref=pay_ref.at[sweep, t], dst_ref=pays_ref.at[sweep, t, :, mine, :],
            send_sem=pay_send.at[sweep, t], recv_sem=pay_recv.at[sweep, t],
            device_id={"cap": lax.rem(me_cap + off, n_cap)}, device_id_type=mesh_id)

    def pay_view(sweep, t):
        return pays_ref.at[sweep, t, :, pl.ds(0, (n_cap - 1) * SLOTS), :]

    def merge(sweep, t):
        pltpu.make_async_copy(pay_view(sweep, t), pay_view(sweep, t), pay_recv.at[sweep, t]).wait()
        hops = n_cap * SLOTS // 8

        def line(i):
            spots = pl.ds(i, 8, stride=hops)
            return pays_ref[sweep, t, 0, spots, :], pays_ref[sweep, t, 1, spots, :]

        def back(at, runs):
            i = hops - 1 - at
            gain, square = line(i)
            points = [gain - square * near[e] for e in range(MERGED_RANGES + 1)]
            for e in range(MERGED_RANGES):
                suf_ref[e, rows_of(i), :] = runs[e + 1]
            return tuple(jnp.maximum(run, point) for run, point in zip(runs, points))

        runs = lax.fori_loop(0, hops, back, (jnp.full((8, 128), NEG, f32),) * (MERGED_RANGES + 1), unroll=8)
        for e in range(MERGED_RANGES + 1):
            tot_ref[e] = runs[e]
        before, after = bases(tot_ref, MERGED_RANGES + 1, sub, 0, 7)

        def ahead(i, carry):
            runs, counts = carry
            gain, square = line(i)
            points = [gain - square * near[e] for e in range(MERGED_RANGES + 1)]
            keep = useful(points, runs, [suf_ref[e, rows_of(i), :] for e in range(MERGED_RANGES)], after)
            runs = tuple(jnp.maximum(run, point) for run, point in zip(runs, points))
            pick_ref[0, rows_of(i), :] = jnp.where(keep, counts, NEG)
            return runs, counts + jnp.where(keep, 1.0, 0.0)

        runs, counts = lax.fori_loop(0, hops, ahead, (tuple(before), jnp.zeros((8, 128), f32)), unroll=8)
        base = counts_before(tot_ref, counts, sub)
        for i in range(hops):
            pick_ref[0, i * 8:(i + 1) * 8, :] = pick_ref[0, i * 8:(i + 1) * 8, :] + base
        spots = [(i, a) for i in range(hops) for a in range(8)]
        picks, squares = collect(
            [(pays_ref[sweep, t, 0, a * hops + i:a * hops + i + 1, :],
              pays_ref[sweep, t, 1, a * hops + i:a * hops + i + 1, :]) for i, a in spots],
            [pick_ref[0, i * 8 + a:i * 8 + a + 1, :] for i, a in spots], MERGED)
        for h in range(-(-MERGED // 8)):
            pick_ref[1, h * 8:(h + 1) * 8, :] = picks[h]
            pick_ref[2, h * 8:(h + 1) * 8, :] = squares[h]
        return jnp.where(base + counts > MERGED, 1.0, 0.0)

    def reply(t):
        gains = [jnp.broadcast_to(pick_ref[1, c:c + 1, :], (8, 128)) for c in range(MERGED)]
        squares = [jnp.broadcast_to(pick_ref[2, c:c + 1, :], (8, 128)) for c in range(MERGED)]

        def one(i, carry):
            rows = rows_of(i)
            slope = col_ref[SLOPE, rows, :]
            capital = col_ref[CAP, rows, :]
            moved = all_max([gain - square * slope for gain, square in zip(gains, squares)])
            best_ref[t, rows, :] = jnp.maximum(moved - 1.41 * capital, g_ref[t, rows, :] - 0.91 * capital)
            return carry

        lax.fori_loop(0, steps, one, 0, unroll=8)

    sums = []
    for t in range(tiles):
        def open_step(i, acc, t=t):
            rows = rows_of(i)
            spots = pl.ds(i, 8, stride=steps)
            mass = jnp.where(exit_rows[t], nat_ref[t, spots, :], 0.0)
            live_ref[t, rows, :] = mass
            value = jnp.where(mass > 0.0, fresh_ref[t, spots, :], 0.3 * col_ref[CAP, rows, :])
            val_ref[t, rows, :] = value
            return acc + weigh(mass, rows, value)

        sums.append(lax.fori_loop(0, steps, open_step, jnp.zeros((8, 128), f32), unroll=16))
    pl.semaphore_wait(barrier, n_dev - 1)
    dem_copies = []
    for off in range(1, n_sec):
        dem_copies.append(pltpu.make_async_remote_copy(
            src_ref=dem_ref, dst_ref=dems_ref.at[pl.ds(me_sec, 1), :], send_sem=dem_send, recv_sem=dem_recv,
            device_id={"sector": lax.rem(me_sec + off, n_sec)}, device_id_type=mesh_id))
        dem_copies[-1].start()
    dems_ref[pl.ds(me_sec, 1), :] = dem_ref[...]
    msg_ref[0, :, lanes:lanes + 128] = jnp.zeros((1, 128), f32)

    def flag_row(flags):
        tot_ref[0] = flags
        return all_max([tot_ref[0, a:a + 1, :] for a in range(8)])

    late = None
    for sweep in range(SWEEPS):
        send_supply(sweep, sums)
        flags = jnp.zeros((8, 128), f32)
        for t in range(tiles):
            forward(t)
            flags = jnp.maximum(flags, prune(sweep, t))
        if sweep == SWEEPS - 1:
            flg_ref[...] = flag_row(flags)

            each_other(lambda device: pltpu.make_async_remote_copy(
                src_ref=flg_ref, dst_ref=flgs_ref.at[pl.ds(my_row, 1), :], send_sem=flg_send, recv_sem=flg_recv,
                device_id=device, device_id_type=mesh_id).start())
            flgs_ref[pl.ds(my_row, 1), :] = flg_ref[...]
        late = jnp.zeros((8, 128), f32)
        for t in range(tiles):
            late = jnp.maximum(late, merge(sweep, t))
            reply(t)
        if sweep == 0:
            msg_ref[1, :, lanes:lanes + 128] = flag_row(jnp.maximum(flags, late))
            wait_rows(n_sec - 1, lanes, dem_recv)
        relative = prices_row(sweep)
        if sweep == 0:
            sums = []
            for t in range(tiles):
                scale = relative[:, t * 128:(t + 1) * 128] * prod_row

                def next_step(i, acc, t=t, scale=scale):
                    rows = rows_of(i)
                    mass = live_ref[t, rows, :]
                    value = jnp.where(mass > 0.0,
                                      scale * col_ref[POW, rows, :] + best_ref[t, rows, :],
                                      0.3 * col_ref[CAP, rows, :])
                    val_ref[t, rows, :] = value
                    return acc + weigh(mass, rows, value)

                sums.append(lax.fori_loop(0, steps, next_step, jnp.zeros((8, 128), f32), unroll=16))
    rel_ref[...] = relative
    for t in range(tiles):
        scale = relative[:, t * 128:(t + 1) * 128] * prod_row

        def last_step(i, carry, t=t, scale=scale):
            rows = rows_of(i)
            out_ref[t, pl.ds(i, 8, stride=steps), :] = jnp.where(
                live_ref[t, rows, :] > 0.0, scale * col_ref[POW, rows, :] + best_ref[t, rows, :],
                0.3 * col_ref[CAP, rows, :])
            return carry

        lax.fori_loop(0, steps, last_step, 0, unroll=8)
    cand_ref[...] = pays_ref[SWEEPS - 1]
    wait_rows(n_dev - 1, 128, flg_recv)
    bad = jnp.max(jnp.maximum(jnp.max(flgs_ref[...], axis=0, keepdims=True),
                              jnp.max(gat_ref[1, :, lanes:lanes + 128], axis=0, keepdims=True)))
    flag_ref[0] = jnp.where(bad > 0.0, 2, jnp.where(jnp.max(late) > 0.0, 1, 0)).astype(jnp.int32)

    for sweep in range(SWEEPS):
        wait_rows(n_dev - 1, lanes + 128, msg_send.at[sweep])
        for t in range(tiles):
            pltpu.make_async_copy(pay_view(sweep, t), pay_view(sweep, t), pay_send.at[sweep, t]).wait()
    wait_rows(n_dev - 1, 128, flg_send)
    wait_rows(n_sec - 1, lanes, dem_send)


def pruned_sweeps(start_value, firm_mass, survive, exit_index, demand, transition, install_cost):
    n_sec, n_cap = lax.axis_size("sector"), lax.axis_size("cap")
    sec_dev, prods, cap_dev = start_value.shape
    lanes = sec_dev * prods
    tiles = lanes // 128
    n_dev = n_sec * n_cap
    far = pl.BlockSpec(memory_space=pl.ANY)
    vmem = pl.BlockSpec(memory_space=pltpu.VMEM)
    smem = pl.BlockSpec(memory_space=pltpu.SMEM)
    f32 = jnp.float32
    dma = pltpu.SemaphoreType.DMA
    pack = max(RANGES, MERGED_RANGES)
    return pl.pallas_call(
        functools.partial(sweeps_kernel, n_sec, n_cap),
        out_shape=(
            jax.ShapeDtypeStruct((tiles, cap_dev, 128), f32),
            jax.ShapeDtypeStruct((tiles, 2, n_cap * SLOTS, 128), f32),
            jax.ShapeDtypeStruct((1, lanes), f32),
            jax.ShapeDtypeStruct((1,), jnp.int32),
        ),
        in_specs=[far] * 7,
        out_specs=(vmem, vmem, vmem, smem),
        scratch_shapes=[
            pltpu.VMEM(start_value.shape, f32),
            pltpu.VMEM(start_value.shape, f32),
            pltpu.VMEM(start_value.shape, jnp.int32),
            pltpu.SMEM((sec_dev,), jnp.int32),
            pltpu.SMEM((sec_dev,), f32),
            pltpu.VMEM((prods, prods), f32),
            pltpu.VMEM((1, cap_dev), f32),
            pltpu.VMEM((tiles, cap_dev, 128), f32),
            pltpu.VMEM((tiles, cap_dev, 128), f32),
            pltpu.VMEM((tiles, cap_dev, 128), f32),
            pltpu.VMEM((tiles, cap_dev, 128), f32),
            pltpu.VMEM((tiles, cap_dev, 128), f32),
            pltpu.VMEM((pack, max(cap_dev, n_cap * SLOTS), 128), f32),
            pltpu.VMEM((tiles, cap_dev, 128), f32),
            pltpu.VMEM((5, cap_dev, 128), f32),
            pltpu.VMEM((RANGES + 1, cap_dev, 128), f32),
            pltpu.VMEM((256, 256), jnp.bfloat16),
            pltpu.VMEM((128, 128), jnp.bfloat16),
            pltpu.VMEM((pack + 1, 8, 128), f32),
            pltpu.VMEM((3, CHUNK_SLOTS * 8, 128), f32),
            pltpu.VMEM((3, max(MERGED, n_cap * SLOTS), 128), f32),
            pltpu.VMEM((tiles * 8, 128), f32),
            pltpu.VMEM((n_sec, lanes), f32),
            pltpu.VMEM((SWEEPS, 1, lanes + 128), f32),
            pltpu.VMEM((SWEEPS, n_dev, lanes + 128), f32),
            pltpu.VMEM((1, lanes), f32),
            pltpu.VMEM((n_sec, lanes), f32),
            pltpu.VMEM((1, 128), f32),
            pltpu.VMEM((n_dev, 128), f32),
            pltpu.VMEM((SWEEPS, tiles, 2, SLOTS, 128), f32),
            pltpu.VMEM((SWEEPS, tiles, 2, n_cap * SLOTS, 128), f32),
            pltpu.VMEM((n_dev - 1, 1, lanes + 128), f32),
            dma((7,)),
            dma((SWEEPS,)), dma((SWEEPS,)), dma, dma, dma, dma,
            dma((SWEEPS, tiles)), dma((SWEEPS, tiles)),
        ],
        compiler_params=pltpu.CompilerParams(
            collective_id=0, has_side_effects=True, vmem_limit_bytes=48 * 1024 * 1024
        ),
    )(start_value, firm_mass, survive, exit_index, demand, transition, install_cost[None, :])


def all_candidates(values, candidates, relative, survive, exit_index):
    sec_dev, prods, cap_dev = values.shape
    total = cap_dev * lax.axis_size("cap")
    capital = capital_of(lax.axis_index("cap") * cap_dev + jnp.arange(cap_dev, dtype=jnp.int32), total)
    prod_index = jnp.arange(prods, dtype=jnp.int32)
    output = jnp.exp(-0.5 + prod_index.astype(jnp.float32) / (prods - 1))[:, None] * capital[None, :] ** 0.6
    live = (survive == 1) & (prod_index[None, :, None] >= exit_index[:, None, None])
    flat = jnp.moveaxis(candidates, 0, 2).reshape(2, candidates.shape[2], sec_dev, prods)

    def one(best, pair):
        return jnp.maximum(best, pair[0][:, :, None] - pair[1][:, :, None] / capital), None

    moved, _ = lax.scan(one, jnp.full(values.shape, NEG, jnp.float32), (flat[0], flat[1]))
    again = relative[:, None, None] * output + (moved - 1.41 * capital)
    return jnp.where(live, jnp.maximum(values, again), values)


def finish_kernel(flipped_ref, row_ref, out_ref, rel_ref):
    tile_sec, prods, cap_dev = out_ref.shape
    lanes, sec_dev = row_ref.shape[1], rel_ref.shape[1]
    for at in range(0, cap_dev, 128):
        out_ref[:, :, at:at + 128] = flipped_ref[0, at:at + 128, :].T.reshape(tile_sec, prods, 128)

    @pl.when(pl.program_id(0) == 0)
    def _():
        column = jnp.sum(jnp.where(
            lax.broadcasted_iota(jnp.int32, (sec_dev, lanes), 1) == prods * lax.broadcasted_iota(
                jnp.int32, (sec_dev, lanes), 0), row_ref[...], 0.0), axis=1, keepdims=True)
        spot = lax.broadcasted_iota(jnp.int32, (sec_dev, sec_dev), 0) == lax.broadcasted_iota(
            jnp.int32, (sec_dev, sec_dev), 1)
        rel_ref[...] = jnp.sum(jnp.where(spot, column, 0.0), axis=0, keepdims=True)


def finish(flipped, row, sec_dev, prods):
    tiles, cap_dev, _ = flipped.shape
    values, relative = pl.pallas_call(
        finish_kernel,
        grid=(tiles,),
        out_shape=(jax.ShapeDtypeStruct((sec_dev, prods, cap_dev), jnp.float32),
                   jax.ShapeDtypeStruct((1, sec_dev), jnp.float32)),
        in_specs=[pl.BlockSpec((1, cap_dev, 128), lambda t: (t, 0, 0)),
                  pl.BlockSpec(row.shape, lambda t: (0, 0))],
        out_specs=(pl.BlockSpec((sec_dev // tiles, prods, cap_dev), lambda t: (t, 0, 0)),
                   pl.BlockSpec((1, sec_dev), lambda t: (0, 0))),
    )(flipped, row)
    return values, relative[0]


def on_device(start_value, firm_mass, survive, exit_index, demand, transition, install_cost):
    args = (start_value, firm_mass, survive, exit_index, demand, transition, install_cost)
    sec_dev, prods, cap_dev = start_value.shape
    if 128 % prods or prods % 8 or sec_dev * prods % 128 or cap_dev % 128 or min(
            lax.axis_size("sector"), lax.axis_size("cap")) < 2:
        return dense_sweeps(*args)
    flipped, candidates, row, state = pruned_sweeps(*args)

    def plain():
        return finish(flipped, row, sec_dev, prods)

    def wide():
        values, relative = plain()
        return all_candidates(values, candidates, relative, survive, exit_index), relative

    return lax.switch(state[0], (plain, wide, lambda: dense_sweeps(*args)))


def solution(mesh):
    return jax.shard_map(
        on_device,
        mesh=mesh,
        in_specs=(
            P("sector", None, "cap"),
            P("sector", None, "cap"),
            P("sector", None, "cap"),
            P("sector"),
            P("sector"),
            P(),
            P("cap"),
        ),
        out_specs=(P("sector", None, "cap"), P("sector")),
        check_vma=False,
    )
```

```python
import functools
import math

import jax
import jax.numpy as jnp
from jax import lax
from jax.experimental import pallas as pl
from jax.experimental.pallas import tpu as pltpu
from jax.sharding import PartitionSpec as P

SWEEPS = 2
CHUNK_SLOTS = 8
SLOTS = 16
MERGED = 12
UNROLLED_DEVICES = 64
RANGES = 4
MERGED_RANGES = 2
NEG = -1e30
LOG_TEN = math.log(10.0)


def capital_of(positions, total):
    return 0.2 * jnp.exp(LOG_TEN * positions.astype(jnp.float32) / (total - 1))


def charge_of(cap_now, cap_next, row_ids, col_ids):
    invest = cap_next - 0.9 * cap_now
    fixed = jnp.where(row_ids == col_ids, 0.0, 1.5 * cap_now)
    return invest + invest * invest / cap_now + fixed


def best_reply(forward_rows, row_first, row_count):
    total_rows, total_cols = forward_rows.shape
    cap_of = functools.partial(capital_of, total=total_cols)
    col_block = math.gcd(total_cols, 2048)
    row_block = math.gcd(row_count, 512)
    grp_limit = max(1, (1 << 24) // (row_block * col_block))
    grp_size = math.gcd(total_rows, 1 << min(total_rows, grp_limit).bit_length() - 1)
    groups = forward_rows.reshape(total_rows // grp_size, grp_size, total_cols)

    def one_group(group):
        row_ids = row_first + jnp.arange(row_count, dtype=jnp.int32)
        cap_rows = cap_of(row_ids)
        col_ids = jnp.arange(total_cols, dtype=jnp.int32)
        cap_cols = cap_of(col_ids)
        charge = charge_of(cap_rows[:, None], cap_cols[None, :], row_ids[:, None], col_ids[None, :])
        return jnp.max(group[:, None, :] - charge[None], axis=2)

    return lax.map(one_group, groups).reshape(total_rows, row_count)


def gather_blocks(block, axis_name):
    count = lax.axis_size(axis_name)
    me = lax.axis_index(axis_name)
    parts = [block]
    for off in range(1, count):
        parts.append(lax.ppermute(block, axis_name, [(d, (d + off) % count) for d in range(count)]))
    return jnp.take(jnp.stack(parts), (me - jnp.arange(count) + count) % count, axis=0)


def dense_sweeps(start_value, firm_mass, survive, exit_index, demand, transition, install_cost):
    sec_dev, prod_count, cap_dev = start_value.shape
    sectors_all = sec_dev * lax.axis_size("sector")
    row_first = lax.axis_index("cap") * cap_dev
    prod_index = jnp.arange(prod_count, dtype=jnp.int32)
    total = cap_dev * lax.axis_size("cap")
    capital = capital_of(row_first + jnp.arange(cap_dev, dtype=jnp.int32), total)
    log_prod = -0.5 + prod_index.astype(jnp.float32) / (prod_count - 1)
    output = jnp.exp(log_prod)[:, None] * capital[None, :] ** 0.6
    scrap = 0.3 * capital
    live = (survive == 1) & (prod_index[None, :, None] >= exit_index[:, None, None])
    values = start_value
    relative = jnp.zeros((sec_dev,), jnp.float32)
    for sweep in range(SWEEPS):
        staying = jnp.where(live, jax.nn.sigmoid((values - scrap) / 0.5), 0.0)
        partial_value = jnp.sum(firm_mass * staying * output, axis=(1, 2))
        supply = 1.0 + jnp.sum(gather_blocks(partial_value, "cap"), axis=0) / (prod_count * total)
        prices = jnp.sqrt(demand / supply)
        root_sum = jnp.sum(gather_blocks(jnp.sqrt(prices), "sector"))
        price_index = (root_sum / sectors_all) ** 2
        relative = prices / price_index
        continuation = jnp.where(live, jnp.maximum(values, scrap), scrap)
        expect = jnp.einsum(
            "zw,swk->szk", transition, continuation, precision=lax.Precision.HIGHEST
        )
        forward_value = 0.9 * expect - install_cost[None, None, :]
        blocks = gather_blocks(forward_value, "cap")
        rows = jnp.moveaxis(blocks, 0, 2).reshape(sec_dev * prod_count, total)
        best = best_reply(rows, row_first, cap_dev).reshape(sec_dev, prod_count, cap_dev)
        values = jnp.where(live, relative[:, None, None] * output + best, scrap)
    return (values, relative)


def rows_of(step):
    return pl.ds(pl.multiple_of(step * 8, 8), 8)


def all_max(parts):
    return functools.reduce(jnp.maximum, parts)


def bases(tot_ref, count, sub, first, last):
    before, after = [], []
    for e in range(count):
        rows = [tot_ref[e, a:a + 1, :] for a in range(8)]
        if e < count - 1:
            before.append(all_max([jnp.where(sub > a, rows[a], NEG) for a in range(7)]))
        if e > 0:
            after.append(all_max([jnp.where(sub < a, rows[a], NEG) for a in range(1, 8)]))
    return before, after


def counts_before(tot_ref, counts, sub):
    tot_ref[0] = counts
    base = jnp.zeros_like(counts)
    for a in range(7):
        base = base + jnp.where(sub > a, tot_ref[0, a:a + 1, :], 0.0)
    return base


def useful(points, runs, sufs, afters):
    keep = None
    for e in range(len(runs)):
        good = (points[e] > runs[e]) & (points[e + 1] > jnp.maximum(sufs[e], afters[e]))
        keep = good if keep is None else keep | good
    return keep


def sweeps_kernel(n_sec, n_cap, start_hbm, mass_hbm, survive_hbm, exit_hbm, demand_hbm, trans_hbm, cost_hbm,
                  out_ref, g_ref, cand_ref, rel_ref, flag_hbm,
                  start_v, mass_v, survive_v, exit_v, demand_v, trans_v, cost_v,
                  nat_ref, fresh_ref, val_ref, live_ref, suf_ref, best_ref, col_ref, qt_ref,
                  weight_ref, ones_ref, tot_ref, l1_ref, pick_ref, zsum_ref, price_ref,
                  msg_ref, gat_ref, dem_ref, dems_ref, pay_ref, pays_ref, size_ref, flag_ref,
                  in_sem, msg_send, msg_recv, dem_send, dem_recv, pay_send, pay_recv):
    sec_dev, prods, cap_dev = start_v.shape
    total = cap_dev * n_cap
    steps = cap_dev // 8
    pitch = steps + 8
    tiles = sec_dev * prods // 128
    tile_sec = 128 // prods
    lanes = tiles * 128
    col_tiles = cap_dev // 128
    n_dev = n_sec * n_cap
    me_cap = lax.axis_index("cap")
    me_sec = lax.axis_index("sector")
    me = me_sec * n_cap + me_cap
    my_row = me_cap * n_sec + me_sec
    mesh_id = pl.DeviceIdType.MESH
    f32 = jnp.float32

    def each_other(act):
        if n_dev > UNROLLED_DEVICES:
            def one(off, carry):
                index = lax.rem(me + off, n_dev)
                act({"sector": index // n_cap, "cap": lax.rem(index, n_cap)})
                return carry

            lax.fori_loop(1, n_dev, one, 0)
            return
        upper = me_sec * 2 // n_sec
        skip = me_sec + upper * (n_sec - 1 - 2 * me_sec)
        for j in range(n_sec - 1):
            spot = n_sec - 1 - j - (j + 1 + skip) // n_sec
            other = spot + upper * (n_sec - 1 - 2 * spot)
            for c in range(n_cap):
                act({"sector": other, "cap": lax.rem(me_cap + c, n_cap)})
        for c in range(1, n_cap):
            act({"sector": me_sec, "cap": lax.rem(me_cap + c, n_cap)})

    loads = []
    for at, (src, dst) in enumerate((
        (trans_hbm, trans_v), (cost_hbm, cost_v), (exit_hbm, exit_v), (demand_hbm, demand_v),
        (mass_hbm, mass_v), (survive_hbm, survive_v), (start_hbm, start_v),
    )):
        loads.append(pltpu.make_async_copy(src, dst, in_sem.at[at]))
        loads[-1].start()

    barrier = pltpu.get_barrier_semaphore()
    each_other(lambda device: pl.semaphore_signal(barrier, inc=1, device_id=device, device_id_type=mesh_id))
    sub = lax.broadcasted_iota(jnp.int32, (8, 128), 0)
    subf = sub.astype(f32)
    lane = lax.broadcasted_iota(jnp.int32, (1, 128), 1)
    lane_prod = lax.rem(lane, prods)
    lane_sec = lane // prods
    ends = [0.5 * 10.0 ** (e / RANGES) for e in range(RANGES + 1)]
    ends[0] *= 1.0 - 1e-5
    ends[-1] *= 1.0 + 1e-5
    first = me_cap * cap_dev
    CAP, SLOPE, POW, GADD, SQUARE = range(5)

    row = lax.broadcasted_iota(jnp.int32, (cap_dev, 128), 0)
    place = first + lax.rem(row, 8) * steps + row // 8
    capital = capital_of(place, total)
    col_ref[CAP] = capital
    col_ref[SLOPE] = 1.0 / capital
    col_ref[POW] = jnp.exp(0.6 * (math.log(0.2) + LOG_TEN * place.astype(f32) / (total - 1)))
    col_ref[SQUARE] = capital * capital
    for e in range(RANGES + 1):
        qt_ref[e] = capital * capital * ends[e]
    edge = [first + cap_dev - 1, first]
    t_low, t_high = [1.0 / capital_of(jnp.full((8, 128), at, jnp.int32), total) for at in edge]
    t_low, t_high = t_low * (1.0 - 1e-5), t_high * (1.0 + 1e-5)
    log_low, log_high = jnp.log(t_low), jnp.log(t_high)
    near = [t_low] + [
        jnp.exp(log_low + (log_high - log_low) * (e / MERGED_RANGES)) for e in range(1, MERGED_RANGES)
    ] + [t_high]
    prod_row = jnp.exp(-0.5 + lane_prod.astype(f32) / (prods - 1))
    big_r = lax.broadcasted_iota(jnp.int32, (128, 128), 0)
    big_c = lax.broadcasted_iota(jnp.int32, (128, 128), 1)
    same = big_r // prods == big_c // prods
    ones_ref[...] = jnp.where(same, 1.0, 0.0).astype(jnp.bfloat16)

    loads[0].wait()
    spot_r = lax.broadcasted_iota(jnp.int32, (128, prods), 0)
    spot_c = lax.broadcasted_iota(jnp.int32, (128, prods), 1)
    spot = jnp.where(lax.rem(spot_r, prods) == spot_c, 1.0, 0.0)
    dims = (((1,), (1,)), ((), ()))
    half = lax.dot_general(spot, trans_v[...], dims, precision=lax.Precision.HIGHEST, preferred_element_type=f32)
    full = lax.dot_general(half, spot, dims, precision=lax.Precision.HIGHEST, preferred_element_type=f32)
    weight = jnp.where(same, 0.9 * full, 0.0)
    top = weight.astype(jnp.bfloat16)
    low = (weight - top.astype(f32)).astype(jnp.bfloat16)
    weight_ref[0:128, 0:128] = top
    weight_ref[128:256, 0:128] = top
    weight_ref[0:128, 128:256] = low
    weight_ref[128:256, 128:256] = jnp.zeros_like(low)

    def place_rows(ref, t, at, block):
        for up in range(0, 128, steps):
            spot = (at + up) // steps * pitch
            ref[t, spot:spot + steps, :] = block[up:up + steps]

    loads[1].wait()
    for at in range(0, cap_dev, 128):
        place_rows(nat_ref, 0, at, jnp.broadcast_to(cost_v[:, at:at + 128], (128, 128)).T)

    def add_step(i, carry):
        rows = rows_of(i)
        col_ref[GADD, rows, :] = 0.8 * col_ref[CAP, rows, :] - nat_ref[0, pl.ds(i, 8, stride=pitch), :]
        return carry

    lax.fori_loop(0, steps, add_step, 0, unroll=8)

    loads[2].wait()
    loads[3].wait()
    exit_rows, demand_rows = [], []
    for t in range(tiles):
        exit_row = jnp.zeros((1, 128), jnp.int32)
        demand_row = jnp.zeros((1, 128), f32)
        for s in range(tile_sec):
            exit_row = jnp.where(lane_sec == s, exit_v[t * tile_sec + s], exit_row)
            demand_row = jnp.where(lane_sec == s, demand_v[t * tile_sec + s], demand_row)
        exit_rows.append(lane_prod >= exit_row)
        demand_rows.append(demand_row)
    dem_ref[...] = jnp.concatenate(demand_rows, axis=1)

    loads[4].wait()
    loads[5].wait()
    for t in range(tiles):
        secs = slice(t * tile_sec, (t + 1) * tile_sec)
        for at in range(0, cap_dev, 128):
            block = jnp.where(survive_v[secs, :, at:at + 128] == 1, mass_v[secs, :, at:at + 128], 0.0)
            place_rows(nat_ref, t, at, block.reshape(128, 128).T)

    loads[6].wait()
    for t in range(tiles):
        secs = slice(t * tile_sec, (t + 1) * tile_sec)
        for at in range(0, cap_dev, 128):
            place_rows(fresh_ref, t, at, start_v[secs, :, at:at + 128].reshape(128, 128).T)

    def weigh(mass, rows, value):
        scrap = 0.3 * col_ref[CAP, rows, :]
        stay = 0.5 + 0.5 * jnp.tanh(value - scrap)
        return mass * stay * col_ref[POW, rows, :]

    def fold_supply(sweep, sums):
        part = jnp.concatenate([one * prod_row for one in sums], axis=0)
        splits = []
        for _ in range(3):
            splits.append(part.astype(jnp.bfloat16).astype(f32))
            part = part - splits[-1]
        grouped = jnp.dot(jnp.concatenate(splits, axis=0).astype(jnp.bfloat16), ones_ref[...],
                          preferred_element_type=f32)
        zsum_ref[...] = grouped[0:tiles * 8] + grouped[tiles * 8:tiles * 16] + grouped[tiles * 16:]
        for t in range(tiles):
            line = zsum_ref[t * 8:t * 8 + 1, :]
            for a in range(1, 8):
                line = line + zsum_ref[t * 8 + a:t * 8 + a + 1, :]
            msg_ref[sweep, :, t * 128:(t + 1) * 128] = line

    def send_supply(sweep):
        each_other(lambda device: pltpu.make_async_remote_copy(
            src_ref=msg_ref.at[sweep], dst_ref=gat_ref.at[sweep, pl.ds(my_row, 1), :],
            send_sem=msg_send.at[sweep], recv_sem=msg_recv.at[sweep],
            device_id=device, device_id_type=mesh_id).start())
        gat_ref[sweep, pl.ds(my_row, 1), :] = msg_ref[sweep]

    def wait_rows(count, width, sem):
        view = size_ref.at[pl.ds(0, count), :, pl.ds(0, width)]
        pltpu.make_async_copy(view, view, sem).wait()

    def prices_row(sweep):
        wait_rows(n_dev - 1, lanes + 128, msg_recv.at[sweep])
        every = gat_ref[sweep, 0:n_sec, 0:lanes]
        for c in range(1, n_cap):
            every = every + gat_ref[sweep, c * n_sec:(c + 1) * n_sec, 0:lanes]
        supply = 1.0 + every / (prods * total)
        prices = jnp.sqrt(dems_ref[...] / supply)
        price_ref[...] = prices
        mean = jnp.sum(jnp.sqrt(prices), keepdims=True) / (lanes * n_sec)
        return price_ref[pl.ds(me_sec, 1), :] / (mean * mean)

    def forward():
        halves = []
        for t in range(tiles):
            cont = jnp.maximum(val_ref[t], 0.3 * col_ref[CAP])
            upper = cont.astype(jnp.bfloat16)
            halves.append(jnp.concatenate([upper, (cont - upper.astype(f32)).astype(jnp.bfloat16)], axis=1))
        both = jnp.dot(jnp.concatenate(halves, axis=0), weight_ref[...], preferred_element_type=f32)
        for t in range(tiles):
            rows = slice(t * cap_dev, (t + 1) * cap_dev)
            g_ref[t] = both[rows, 0:128] + both[rows, 128:256] + col_ref[GADD]

    def collect(rows_list, rank_rows, count):
        picks = [jnp.full((8, 128), NEG, f32) for _ in range(-(-count // 8))]
        squares = [jnp.zeros((8, 128), f32) for _ in range(-(-count // 8))]
        for (gain, square), rank in zip(rows_list, rank_rows):
            for h in range(-(-count // 8)):
                here = rank == subf + 8.0 * h
                picks[h] = jnp.where(here, gain, picks[h])
                squares[h] = jnp.where(here, square, squares[h])
        return picks, squares

    def prune(sweep, t):
        def back(at, runs):
            i = steps - 1 - at
            rows = rows_of(i)
            gain = g_ref[t, rows, :]
            points = [gain - qt_ref[e, rows, :] for e in range(RANGES + 1)]
            for e in range(RANGES):
                suf_ref[e, rows, :] = runs[e + 1]
            return tuple(jnp.maximum(run, point) for run, point in zip(runs, points))

        runs = lax.fori_loop(0, steps, back, (jnp.full((8, 128), NEG, f32),) * (RANGES + 1), unroll=16)
        for e in range(RANGES + 1):
            tot_ref[e] = runs[e]
        before, after = bases(tot_ref, RANGES + 1, sub, 0, 7)

        def ahead(i, carry):
            runs, counts, gains, squares = carry
            rows = rows_of(i)
            gain = g_ref[t, rows, :]
            square = col_ref[SQUARE, rows, :]
            points = [gain - qt_ref[e, rows, :] for e in range(RANGES + 1)]
            keep = useful(points, runs, [suf_ref[e, rows, :] for e in range(RANGES)], after)
            runs = tuple(jnp.maximum(run, point) for run, point in zip(runs, points))
            gains = tuple(jnp.where(keep, new, old) for new, old in zip((gain,) + gains, gains))
            squares = tuple(jnp.where(keep, new, old) for new, old in zip((square,) + squares, squares))
            return runs, counts + jnp.where(keep, 1.0, 0.0), gains, squares

        zero = jnp.zeros((8, 128), f32)
        runs, counts, gains, squares = lax.fori_loop(
            0, steps, ahead, (tuple(before), zero, (zero,) * CHUNK_SLOTS, (zero,) * CHUNK_SLOTS), unroll=8)
        base = counts_before(tot_ref, counts, sub)
        for p in range(CHUNK_SLOTS):
            l1_ref[0, p * 8:(p + 1) * 8, :] = gains[p]
            l1_ref[1, p * 8:(p + 1) * 8, :] = squares[p]
            l1_ref[2, p * 8:(p + 1) * 8, :] = jnp.where(counts > p, base + counts - (p + 1.0), -1.0)
        spots = range(CHUNK_SLOTS * 8)
        picks, squares = collect(
            [(l1_ref[0, r:r + 1, :], l1_ref[1, r:r + 1, :]) for r in spots],
            [l1_ref[2, r:r + 1, :] for r in spots], SLOTS)
        over = flag_row(jnp.where((counts > CHUNK_SLOTS) | (base + counts > SLOTS), 1.0, 0.0))
        for h in range(SLOTS // 8):
            pay_ref[sweep, t, 0, h * 8:(h + 1) * 8, :] = picks[h]
            pay_ref[sweep, t, 1, h * 8:(h + 1) * 8, :] = jnp.where(over > 0.0, -1.0, squares[h])

    def send_payment(sweep, t):
        mine = pl.ds(pl.multiple_of(me_cap * SLOTS, SLOTS), SLOTS)
        for off in range(1, n_cap):
            payment(sweep, t, off).start()
        pays_ref[sweep, t, :, mine, :] = pay_ref[sweep, t]

    def flag_row(flags):
        tot_ref[0] = flags
        return all_max([tot_ref[0, a:a + 1, :] for a in range(8)])

    def payment(sweep, t, off):
        mine = pl.ds(pl.multiple_of(me_cap * SLOTS, SLOTS), SLOTS)
        return pltpu.make_async_remote_copy(
            src_ref=pay_ref.at[sweep, t], dst_ref=pays_ref.at[sweep, t, :, mine, :],
            send_sem=pay_send.at[sweep, t], recv_sem=pay_recv.at[sweep, t],
            device_id={"cap": lax.rem(me_cap + off, n_cap)}, device_id_type=mesh_id)

    def pay_view(sweep, t):
        return pays_ref.at[sweep, t, :, pl.ds(0, (n_cap - 1) * SLOTS), :]

    def merge(sweep, t):
        pltpu.make_async_copy(pay_view(sweep, t), pay_view(sweep, t), pay_recv.at[sweep, t]).wait()
        hops = n_cap * SLOTS // 8

        def line(i):
            spots = pl.ds(i, 8, stride=hops)
            return pays_ref[sweep, t, 0, spots, :], pays_ref[sweep, t, 1, spots, :]

        def back(at, runs):
            i = hops - 1 - at
            gain, square = line(i)
            points = [gain - square * near[e] for e in range(MERGED_RANGES + 1)]
            for e in range(MERGED_RANGES):
                suf_ref[e, rows_of(i), :] = runs[e + 1]
            return tuple(jnp.maximum(run, point) for run, point in zip(runs, points))

        runs = lax.fori_loop(0, hops, back, (jnp.full((8, 128), NEG, f32),) * (MERGED_RANGES + 1), unroll=8)
        for e in range(MERGED_RANGES + 1):
            tot_ref[e] = runs[e]
        before, after = bases(tot_ref, MERGED_RANGES + 1, sub, 0, 7)

        def ahead(i, carry):
            runs, counts, lost = carry
            gain, square = line(i)
            points = [gain - square * near[e] for e in range(MERGED_RANGES + 1)]
            keep = useful(points, runs, [suf_ref[e, rows_of(i), :] for e in range(MERGED_RANGES)], after)
            runs = tuple(jnp.maximum(run, point) for run, point in zip(runs, points))
            pick_ref[0, rows_of(i), :] = jnp.where(keep, counts, NEG)
            return runs, counts + jnp.where(keep, 1.0, 0.0), jnp.minimum(lost, square)

        zero = jnp.zeros((8, 128), f32)
        runs, counts, lost = lax.fori_loop(0, hops, ahead, (tuple(before), zero, zero), unroll=8)
        base = counts_before(tot_ref, counts, sub)
        for i in range(hops):
            pick_ref[0, i * 8:(i + 1) * 8, :] = pick_ref[0, i * 8:(i + 1) * 8, :] + base
        spots = [(i, a) for i in range(hops) for a in range(8)]
        picks, squares = collect(
            [(pays_ref[sweep, t, 0, a * hops + i:a * hops + i + 1, :],
              pays_ref[sweep, t, 1, a * hops + i:a * hops + i + 1, :]) for i, a in spots],
            [pick_ref[0, i * 8 + a:i * 8 + a + 1, :] for i, a in spots], MERGED)
        for h in range(-(-MERGED // 8)):
            pick_ref[1, h * 8:(h + 1) * 8, :] = picks[h]
            pick_ref[2, h * 8:(h + 1) * 8, :] = squares[h]
        return jnp.where(lost < 0.0, 2.0, jnp.where(base + counts > MERGED, 1.0, 0.0))

    def reply(t):
        gains = [jnp.broadcast_to(pick_ref[1, c:c + 1, :], (8, 128)) for c in range(MERGED)]
        squares = [jnp.broadcast_to(pick_ref[2, c:c + 1, :], (8, 128)) for c in range(MERGED)]

        def one(i, carry):
            rows = rows_of(i)
            slope = col_ref[SLOPE, rows, :]
            capital = col_ref[CAP, rows, :]
            moved = all_max([gain - square * slope for gain, square in zip(gains, squares)])
            best_ref[t, rows, :] = jnp.maximum(moved - 1.41 * capital, g_ref[t, rows, :] - 0.91 * capital)
            return carry

        lax.fori_loop(0, steps, one, 0, unroll=8)

    sums = []
    for t in range(tiles):
        def open_step(i, acc, t=t):
            rows = rows_of(i)
            spots = pl.ds(i, 8, stride=pitch)
            mass = jnp.where(exit_rows[t], nat_ref[t, spots, :], 0.0)
            live_ref[t, rows, :] = mass
            value = jnp.where(mass > 0.0, fresh_ref[t, spots, :], 0.3 * col_ref[CAP, rows, :])
            val_ref[t, rows, :] = value
            return acc + weigh(mass, rows, value)

        sums.append(lax.fori_loop(0, steps, open_step, jnp.zeros((8, 128), f32), unroll=16))
    msg_ref[0, :, lanes:lanes + 128] = jnp.zeros((1, 128), f32)
    dem_copies = [pltpu.make_async_remote_copy(
        src_ref=dem_ref, dst_ref=dems_ref.at[pl.ds(me_sec, 1), :], send_sem=dem_send, recv_sem=dem_recv,
        device_id={"sector": lax.rem(me_sec + off, n_sec)}, device_id_type=mesh_id) for off in range(1, n_sec)]
    dems_ref[pl.ds(me_sec, 1), :] = dem_ref[...]
    state = jnp.zeros((8, 128), f32)
    for sweep in range(SWEEPS):
        fold_supply(sweep, sums)
        if sweep > 0:
            send_supply(sweep)
        forward()
        for t in range(tiles):
            prune(sweep, t)
            if sweep == 0 and t == 0:
                pl.semaphore_wait(barrier, n_dev - 1)
                send_supply(sweep)
                for copy in dem_copies:
                    copy.start()
            send_payment(sweep, t)
        for t in range(tiles):
            state = jnp.maximum(state, merge(sweep, t))
            reply(t)
        if sweep == 0:
            msg_ref[1, :, lanes:lanes + 128] = flag_row(state)
            state = jnp.zeros((8, 128), f32)
            wait_rows(n_sec - 1, lanes, dem_recv)
        relative = prices_row(sweep)
        if sweep == 0:
            sums = []
            for t in range(tiles):
                scale = relative[:, t * 128:(t + 1) * 128] * prod_row

                def next_step(i, acc, t=t, scale=scale):
                    rows = rows_of(i)
                    mass = live_ref[t, rows, :]
                    value = jnp.where(mass > 0.0,
                                      scale * col_ref[POW, rows, :] + best_ref[t, rows, :],
                                      0.3 * col_ref[CAP, rows, :])
                    val_ref[t, rows, :] = value
                    return acc + weigh(mass, rows, value)

                sums.append(lax.fori_loop(0, steps, next_step, jnp.zeros((8, 128), f32), unroll=16))
    rel_ref[...] = relative
    early = jnp.max(gat_ref[1, :, lanes:lanes + 128], axis=0, keepdims=True)
    flag_ref[0] = jnp.max(jnp.maximum(state, jnp.where(early > 0.0, 3.0, 0.0))).astype(jnp.int32)
    report = pltpu.make_async_copy(flag_ref, flag_hbm, in_sem.at[0])
    report.start()
    for t in range(tiles):
        scale = relative[:, t * 128:(t + 1) * 128] * prod_row

        def last_step(i, carry, t=t, scale=scale):
            rows = rows_of(i)
            out_ref[t, pl.ds(i, 8, stride=pitch), :] = jnp.where(
                live_ref[t, rows, :] > 0.0, scale * col_ref[POW, rows, :] + best_ref[t, rows, :],
                0.3 * col_ref[CAP, rows, :])
            return carry

        lax.fori_loop(0, steps, last_step, 0, unroll=8)
    cand_ref[...] = pays_ref[SWEEPS - 1]
    for sweep in range(SWEEPS):
        wait_rows(n_dev - 1, lanes + 128, msg_send.at[sweep])
        for t in range(tiles):
            pltpu.make_async_copy(pay_view(sweep, t), pay_view(sweep, t), pay_send.at[sweep, t]).wait()
    wait_rows(n_sec - 1, lanes, dem_send)
    report.wait()


def pruned_sweeps(start_value, firm_mass, survive, exit_index, demand, transition, install_cost):
    n_sec, n_cap = lax.axis_size("sector"), lax.axis_size("cap")
    sec_dev, prods, cap_dev = start_value.shape
    lanes = sec_dev * prods
    tiles = lanes // 128
    n_dev = n_sec * n_cap
    far = pl.BlockSpec(memory_space=pl.ANY)
    vmem = pl.BlockSpec(memory_space=pltpu.VMEM)
    smem = pl.BlockSpec(memory_space=pltpu.SMEM)
    f32 = jnp.float32
    dma = pltpu.SemaphoreType.DMA
    pack = max(RANGES, MERGED_RANGES)
    return pl.pallas_call(
        functools.partial(sweeps_kernel, n_sec, n_cap),
        out_shape=(
            jax.ShapeDtypeStruct((tiles, cap_dev + 64, 128), f32),
            jax.ShapeDtypeStruct((tiles, cap_dev, 128), f32),
            jax.ShapeDtypeStruct((tiles, 2, n_cap * SLOTS, 128), f32),
            jax.ShapeDtypeStruct((1, lanes), f32),
            jax.ShapeDtypeStruct((1,), jnp.int32),
        ),
        in_specs=[far] * 7,
        out_specs=(vmem, vmem, vmem, vmem, far),
        scratch_shapes=[
            pltpu.VMEM(start_value.shape, f32),
            pltpu.VMEM(start_value.shape, f32),
            pltpu.VMEM(start_value.shape, jnp.int32),
            pltpu.SMEM((sec_dev,), jnp.int32),
            pltpu.SMEM((sec_dev,), f32),
            pltpu.VMEM((prods, prods), f32),
            pltpu.VMEM((1, cap_dev), f32),
            pltpu.VMEM((tiles, cap_dev + 64, 128), f32),
            pltpu.VMEM((tiles, cap_dev + 64, 128), f32),
            pltpu.VMEM((tiles, cap_dev, 128), f32),
            pltpu.VMEM((tiles, cap_dev, 128), f32),
            pltpu.VMEM((pack, max(cap_dev, n_cap * SLOTS), 128), f32),
            pltpu.VMEM((tiles, cap_dev, 128), f32),
            pltpu.VMEM((5, cap_dev, 128), f32),
            pltpu.VMEM((RANGES + 1, cap_dev, 128), f32),
            pltpu.VMEM((256, 256), jnp.bfloat16),
            pltpu.VMEM((128, 128), jnp.bfloat16),
            pltpu.VMEM((pack + 1, 8, 128), f32),
            pltpu.VMEM((3, CHUNK_SLOTS * 8, 128), f32),
            pltpu.VMEM((3, max(MERGED, n_cap * SLOTS), 128), f32),
            pltpu.VMEM((tiles * 8, 128), f32),
            pltpu.VMEM((n_sec, lanes), f32),
            pltpu.VMEM((SWEEPS, 1, lanes + 128), f32),
            pltpu.VMEM((SWEEPS, n_dev, lanes + 128), f32),
            pltpu.VMEM((1, lanes), f32),
            pltpu.VMEM((n_sec, lanes), f32),
            pltpu.VMEM((SWEEPS, tiles, 2, SLOTS, 128), f32),
            pltpu.VMEM((SWEEPS, tiles, 2, n_cap * SLOTS, 128), f32),
            pltpu.VMEM((n_dev - 1, 1, lanes + 128), f32),
            pltpu.SMEM((1,), jnp.int32),
            dma((7,)),
            dma((SWEEPS,)), dma((SWEEPS,)), dma, dma,
            dma((SWEEPS, tiles)), dma((SWEEPS, tiles)),
        ],
        compiler_params=pltpu.CompilerParams(
            collective_id=0, has_side_effects=True, vmem_limit_bytes=48 * 1024 * 1024
        ),
    )(start_value, firm_mass, survive, exit_index, demand, transition, install_cost[None, :])


def all_candidates(values, candidates, relative, survive, exit_index):
    sec_dev, prods, cap_dev = values.shape
    total = cap_dev * lax.axis_size("cap")
    capital = capital_of(lax.axis_index("cap") * cap_dev + jnp.arange(cap_dev, dtype=jnp.int32), total)
    prod_index = jnp.arange(prods, dtype=jnp.int32)
    output = jnp.exp(-0.5 + prod_index.astype(jnp.float32) / (prods - 1))[:, None] * capital[None, :] ** 0.6
    live = (survive == 1) & (prod_index[None, :, None] >= exit_index[:, None, None])
    flat = jnp.moveaxis(candidates, 0, 2).reshape(2, candidates.shape[2], sec_dev, prods)

    def one(best, pair):
        return jnp.maximum(best, pair[0][:, :, None] - pair[1][:, :, None] / capital), None

    moved, _ = lax.scan(one, jnp.full(values.shape, NEG, jnp.float32), (flat[0], flat[1]))
    again = relative[:, None, None] * output + (moved - 1.41 * capital)
    return jnp.where(live, jnp.maximum(values, again), values)


def group_sweep(gains, relative, survive, exit_index):
    sec_dev, prods, cap_dev = survive.shape
    tiles = gains.shape[0]
    total = cap_dev * lax.axis_size("cap")
    row_first = lax.axis_index("cap") * cap_dev
    capital = capital_of(row_first + jnp.arange(cap_dev, dtype=jnp.int32), total)
    prod_index = jnp.arange(prods, dtype=jnp.int32)
    output = jnp.exp(-0.5 + prod_index.astype(jnp.float32) / (prods - 1))[:, None] * capital[None, :] ** 0.6
    live = (survive == 1) & (prod_index[None, :, None] >= exit_index[:, None, None])
    natural = gains.reshape(tiles, cap_dev // 8, 8, 128).swapaxes(1, 2).reshape(tiles, cap_dev, 128)
    forward_value = natural.swapaxes(1, 2).reshape(sec_dev, prods, cap_dev) - 0.8 * capital
    rows = jnp.moveaxis(gather_blocks(forward_value, "cap"), 0, 2).reshape(sec_dev * prods, total)
    best = best_reply(rows, row_first, cap_dev).reshape(sec_dev, prods, cap_dev)
    return jnp.where(live, relative[:, None, None] * output + best, 0.3 * capital)


def finish_kernel(flipped_ref, row_ref, out_ref, rel_ref):
    tile_sec, prods, cap_dev = out_ref.shape
    lanes, sec_dev = row_ref.shape[1], rel_ref.shape[1]
    steps = cap_dev // 8
    for at in range(0, cap_dev, 128):
        spots = [(at + up) // steps * (steps + 8) for up in range(0, 128, steps)]
        block = jnp.concatenate([flipped_ref[0, spot:spot + steps, :] for spot in spots], axis=0)
        out_ref[:, :, at:at + 128] = block.T.reshape(tile_sec, prods, 128)

    @pl.when(pl.program_id(0) == 0)
    def _():
        column = jnp.sum(jnp.where(
            lax.broadcasted_iota(jnp.int32, (sec_dev, lanes), 1) == prods * lax.broadcasted_iota(
                jnp.int32, (sec_dev, lanes), 0), row_ref[...], 0.0), axis=1, keepdims=True)
        spot = lax.broadcasted_iota(jnp.int32, (sec_dev, sec_dev), 0) == lax.broadcasted_iota(
            jnp.int32, (sec_dev, sec_dev), 1)
        rel_ref[...] = jnp.sum(jnp.where(spot, column, 0.0), axis=0, keepdims=True)


def finish(flipped, row, sec_dev, prods):
    tiles, padded, _ = flipped.shape
    cap_dev = padded - 64
    values, relative = pl.pallas_call(
        finish_kernel,
        grid=(tiles,),
        out_shape=(jax.ShapeDtypeStruct((sec_dev, prods, cap_dev), jnp.float32),
                   jax.ShapeDtypeStruct((1, sec_dev), jnp.float32)),
        in_specs=[pl.BlockSpec((1, padded, 128), lambda t: (t, 0, 0)),
                  pl.BlockSpec(row.shape, lambda t: (0, 0))],
        out_specs=(pl.BlockSpec((sec_dev // tiles, prods, cap_dev), lambda t: (t, 0, 0)),
                   pl.BlockSpec((1, sec_dev), lambda t: (0, 0))),
    )(flipped, row)
    return values, relative[0]


def on_device(start_value, firm_mass, survive, exit_index, demand, transition, install_cost):
    args = (start_value, firm_mass, survive, exit_index, demand, transition, install_cost)
    sec_dev, prods, cap_dev = start_value.shape
    if 128 % prods or prods % 8 or sec_dev * prods % 128 or cap_dev % 128 or min(
            lax.axis_size("sector"), lax.axis_size("cap")) < 2:
        return dense_sweeps(*args)
    flipped, gains, candidates, row, state = pruned_sweeps(*args)

    def plain():
        return finish(flipped, row, sec_dev, prods)

    def wide():
        values, relative = plain()
        return all_candidates(values, candidates, relative, survive, exit_index), relative

    def group():
        relative = row.reshape(sec_dev, prods)[:, 0]
        return group_sweep(gains, relative, survive, exit_index), relative

    return lax.switch(state[0], (plain, wide, group, lambda: dense_sweeps(*args)))


def solution(mesh):
    return jax.shard_map(
        on_device,
        mesh=mesh,
        in_specs=(
            P("sector", None, "cap"),
            P("sector", None, "cap"),
            P("sector", None, "cap"),
            P("sector"),
            P("sector"),
            P(),
            P("cap"),
        ),
        out_specs=(P("sector", None, "cap"), P("sector")),
        check_vma=False,
    )
```

```python
import functools
import math

import jax
import jax.numpy as jnp
from jax import lax
from jax.experimental import pallas as pl
from jax.experimental.pallas import tpu as pltpu
from jax.sharding import PartitionSpec as P

SWEEPS = 2
CHUNK_SLOTS = 8
SLOTS = 16
MERGED = 12
UNROLLED_DEVICES = 64
RANGES = 4
MERGED_RANGES = 2
NEG = -1e30
LOG_TEN = math.log(10.0)


def capital_of(positions, total):
    return 0.2 * jnp.exp(LOG_TEN * positions.astype(jnp.float32) / (total - 1))


def charge_of(cap_now, cap_next, row_ids, col_ids):
    invest = cap_next - 0.9 * cap_now
    fixed = jnp.where(row_ids == col_ids, 0.0, 1.5 * cap_now)
    return invest + invest * invest / cap_now + fixed


def best_reply(forward_rows, row_first, row_count):
    total_rows, total_cols = forward_rows.shape
    cap_of = functools.partial(capital_of, total=total_cols)
    col_block = math.gcd(total_cols, 2048)
    row_block = math.gcd(row_count, 512)
    grp_limit = max(1, (1 << 24) // (row_block * col_block))
    grp_size = math.gcd(total_rows, 1 << min(total_rows, grp_limit).bit_length() - 1)
    groups = forward_rows.reshape(total_rows // grp_size, grp_size, total_cols)

    def one_group(group):
        row_ids = row_first + jnp.arange(row_count, dtype=jnp.int32)
        cap_rows = cap_of(row_ids)
        col_ids = jnp.arange(total_cols, dtype=jnp.int32)
        cap_cols = cap_of(col_ids)
        charge = charge_of(cap_rows[:, None], cap_cols[None, :], row_ids[:, None], col_ids[None, :])
        return jnp.max(group[:, None, :] - charge[None], axis=2)

    return lax.map(one_group, groups).reshape(total_rows, row_count)


def gather_blocks(block, axis_name):
    count = lax.axis_size(axis_name)
    me = lax.axis_index(axis_name)
    parts = [block]
    for off in range(1, count):
        parts.append(lax.ppermute(block, axis_name, [(d, (d + off) % count) for d in range(count)]))
    return jnp.take(jnp.stack(parts), (me - jnp.arange(count) + count) % count, axis=0)


def dense_sweeps(start_value, firm_mass, survive, exit_index, demand, transition, install_cost):
    sec_dev, prod_count, cap_dev = start_value.shape
    sectors_all = sec_dev * lax.axis_size("sector")
    row_first = lax.axis_index("cap") * cap_dev
    prod_index = jnp.arange(prod_count, dtype=jnp.int32)
    total = cap_dev * lax.axis_size("cap")
    capital = capital_of(row_first + jnp.arange(cap_dev, dtype=jnp.int32), total)
    log_prod = -0.5 + prod_index.astype(jnp.float32) / (prod_count - 1)
    output = jnp.exp(log_prod)[:, None] * capital[None, :] ** 0.6
    scrap = 0.3 * capital
    live = (survive == 1) & (prod_index[None, :, None] >= exit_index[:, None, None])
    values = start_value
    relative = jnp.zeros((sec_dev,), jnp.float32)
    for sweep in range(SWEEPS):
        staying = jnp.where(live, jax.nn.sigmoid((values - scrap) / 0.5), 0.0)
        partial_value = jnp.sum(firm_mass * staying * output, axis=(1, 2))
        supply = 1.0 + jnp.sum(gather_blocks(partial_value, "cap"), axis=0) / (prod_count * total)
        prices = jnp.sqrt(demand / supply)
        root_sum = jnp.sum(gather_blocks(jnp.sqrt(prices), "sector"))
        price_index = (root_sum / sectors_all) ** 2
        relative = prices / price_index
        continuation = jnp.where(live, jnp.maximum(values, scrap), scrap)
        expect = jnp.einsum(
            "zw,swk->szk", transition, continuation, precision=lax.Precision.HIGHEST
        )
        forward_value = 0.9 * expect - install_cost[None, None, :]
        blocks = gather_blocks(forward_value, "cap")
        rows = jnp.moveaxis(blocks, 0, 2).reshape(sec_dev * prod_count, total)
        best = best_reply(rows, row_first, cap_dev).reshape(sec_dev, prod_count, cap_dev)
        values = jnp.where(live, relative[:, None, None] * output + best, scrap)
    return (values, relative)


def rows_of(step):
    return pl.ds(pl.multiple_of(step * 8, 8), 8)


def all_max(parts):
    return functools.reduce(jnp.maximum, parts)


def bases(tot_ref, count, sub):
    before, after = [], []
    for e in range(count):
        rows = [tot_ref[e, a:a + 1, :] for a in range(8)]
        if e < count - 1:
            before.append(all_max([jnp.where(sub > a, rows[a], NEG) for a in range(7)]))
        if e > 0:
            after.append(all_max([jnp.where(sub < a, rows[a], NEG) for a in range(1, 8)]))
    return before, after


def counts_before(tot_ref, counts, sub):
    tot_ref[0] = counts
    base = jnp.zeros_like(counts)
    for a in range(7):
        base = base + jnp.where(sub > a, tot_ref[0, a:a + 1, :], 0.0)
    return base


def useful(points, runs, sufs, afters):
    keep = None
    for e in range(len(runs)):
        good = (points[e] > runs[e]) & (points[e + 1] > jnp.maximum(sufs[e], afters[e]))
        keep = good if keep is None else keep | good
    return keep


def sweeps_kernel(n_sec, n_cap, start_hbm, mass_hbm, survive_hbm, exit_hbm, demand_hbm, trans_hbm, cost_hbm,
                  out_ref, g_ref, cand_ref, rel_ref, flag_hbm,
                  start_v, mass_v, survive_v, exit_v, demand_v, trans_v, cost_v,
                  nat_ref, fresh_ref, val_ref, live_ref, pre_ref, ends_ref, suf_ref, best_ref, col_ref, qt_ref,
                  weight_ref, ones_ref, tot_ref, l1_ref, pick_ref, zsum_ref, price_ref,
                  msg_ref, gat_ref, dem_ref, dems_ref, pay_ref, pays_ref, size_ref, flag_ref,
                  in_sem, msg_send, msg_recv, dem_send, dem_recv, pay_send, pay_recv):
    sec_dev, prods, cap_dev = start_v.shape
    total = cap_dev * n_cap
    steps = cap_dev // 8
    pitch = steps + 8
    tiles = sec_dev * prods // 128
    tile_sec = 128 // prods
    lanes = tiles * 128
    col_tiles = cap_dev // 128
    n_dev = n_sec * n_cap
    me_cap = lax.axis_index("cap")
    me_sec = lax.axis_index("sector")
    me = me_sec * n_cap + me_cap
    my_row = me_cap * n_sec + me_sec
    mesh_id = pl.DeviceIdType.MESH
    f32 = jnp.float32

    def each_other(act, far=True, close=True):
        if n_dev > UNROLLED_DEVICES:
            if not far:
                return

            def one(off, carry):
                index = lax.rem(me + off, n_dev)
                act({"sector": index // n_cap, "cap": lax.rem(index, n_cap)})
                return carry

            lax.fori_loop(1, n_dev, one, 0)
            return
        upper = me_sec * 2 // n_sec
        skip = me_sec + upper * (n_sec - 1 - 2 * me_sec)
        for j in range(0 if far else n_sec // 2, n_sec - 1 if close else n_sec // 2):
            spot = n_sec - 1 - j - (j + 1 + skip) // n_sec
            other = spot + upper * (n_sec - 1 - 2 * spot)
            for c in range(n_cap):
                act({"sector": other, "cap": lax.rem(me_cap + c, n_cap)})
        for c in range(1, n_cap if close else 1):
            act({"sector": me_sec, "cap": lax.rem(me_cap + c, n_cap)})

    loads = []
    for at, (src, dst) in enumerate((
        (trans_hbm, trans_v), (cost_hbm, cost_v), (exit_hbm, exit_v), (demand_hbm, demand_v),
        (mass_hbm, mass_v), (survive_hbm, survive_v), (start_hbm, start_v),
    )):
        loads.append(pltpu.make_async_copy(src, dst, in_sem.at[at]))
        loads[-1].start()

    barrier = pltpu.get_barrier_semaphore()
    each_other(lambda device: pl.semaphore_signal(barrier, inc=1, device_id=device, device_id_type=mesh_id))
    sub = lax.broadcasted_iota(jnp.int32, (8, 128), 0)
    subf = sub.astype(f32)
    lane = lax.broadcasted_iota(jnp.int32, (1, 128), 1)
    lane_prod = lax.rem(lane, prods)
    lane_sec = lane // prods
    ends = [0.5 * 10.0 ** (e / RANGES) for e in range(RANGES + 1)]
    ends[0] *= 1.0 - 1e-5
    ends[-1] *= 1.0 + 1e-5
    first = me_cap * cap_dev
    CAP, SLOPE, POW, GADD, SQUARE = range(5)

    row = lax.broadcasted_iota(jnp.int32, (cap_dev, 128), 0)
    place = first + lax.rem(row, 8) * steps + row // 8
    capital = capital_of(place, total)
    col_ref[CAP] = capital
    col_ref[SLOPE] = 1.0 / capital
    col_ref[POW] = jnp.exp(0.6 * (math.log(0.2) + LOG_TEN * place.astype(f32) / (total - 1)))
    col_ref[SQUARE] = capital * capital
    for e in range(RANGES + 1):
        qt_ref[e] = capital * capital * ends[e]
    edge = [first + cap_dev - 1, first]
    t_low, t_high = [1.0 / capital_of(jnp.full((8, 128), at, jnp.int32), total) for at in edge]
    t_low, t_high = t_low * (1.0 - 1e-5), t_high * (1.0 + 1e-5)
    log_low, log_high = jnp.log(t_low), jnp.log(t_high)
    near = [t_low] + [
        jnp.exp(log_low + (log_high - log_low) * (e / MERGED_RANGES)) for e in range(1, MERGED_RANGES)
    ] + [t_high]
    prod_row = jnp.exp(-0.5 + lane_prod.astype(f32) / (prods - 1))
    big_r = lax.broadcasted_iota(jnp.int32, (128, 128), 0)
    big_c = lax.broadcasted_iota(jnp.int32, (128, 128), 1)
    same = big_r // prods == big_c // prods
    ones_ref[...] = jnp.where(same, 1.0, 0.0).astype(jnp.bfloat16)

    loads[0].wait()
    spot_r = lax.broadcasted_iota(jnp.int32, (128, prods), 0)
    spot_c = lax.broadcasted_iota(jnp.int32, (128, prods), 1)
    spot = jnp.where(lax.rem(spot_r, prods) == spot_c, 1.0, 0.0).astype(jnp.bfloat16)
    scaled = 0.9 * trans_v[...]
    upper = scaled.astype(jnp.bfloat16)
    pair = jnp.concatenate([upper, (scaled - upper.astype(f32)).astype(jnp.bfloat16)], axis=0)
    half = lax.dot_general(spot, pair, (((1,), (1,)), ((), ())), preferred_element_type=f32)
    fan_r = lax.broadcasted_iota(jnp.int32, (2 * prods, 256), 0)
    fan_c = lax.broadcasted_iota(jnp.int32, (2 * prods, 256), 1)
    fan = (lax.rem(fan_r, prods) == lax.rem(fan_c, prods)) & (fan_r // prods == fan_c // 128)
    full = jnp.dot(half.astype(jnp.bfloat16), jnp.where(fan, 1.0, 0.0).astype(jnp.bfloat16), preferred_element_type=f32)
    top = jnp.where(same, full[:, 0:128], 0.0).astype(jnp.bfloat16)
    low = jnp.where(same, full[:, 128:256], 0.0).astype(jnp.bfloat16)
    weight_ref[0:128, 0:128] = top
    weight_ref[128:256, 0:128] = top
    weight_ref[0:128, 128:256] = low
    weight_ref[128:256, 128:256] = jnp.zeros_like(low)

    def place_rows(ref, t, at, block):
        for up in range(0, 128, steps):
            spot = (at + up) // steps * pitch
            ref[t, spot:spot + steps, :] = block[up:up + steps]

    loads[1].wait()
    for at in range(0, cap_dev, 128):
        place_rows(nat_ref, 0, at, jnp.broadcast_to(cost_v[:, at:at + 128], (128, 128)).T)

    def add_step(i, carry):
        rows = rows_of(i)
        col_ref[GADD, rows, :] = 0.8 * col_ref[CAP, rows, :] - nat_ref[0, pl.ds(i, 8, stride=pitch), :]
        return carry

    lax.fori_loop(0, steps, add_step, 0, unroll=8)

    loads[2].wait()
    loads[3].wait()
    exit_rows, demand_rows = [], []
    for t in range(tiles):
        exit_row = jnp.zeros((1, 128), jnp.int32)
        demand_row = jnp.zeros((1, 128), f32)
        for s in range(tile_sec):
            exit_row = jnp.where(lane_sec == s, exit_v[t * tile_sec + s], exit_row)
            demand_row = jnp.where(lane_sec == s, demand_v[t * tile_sec + s], demand_row)
        exit_rows.append(lane_prod >= exit_row)
        demand_rows.append(demand_row)
    dem_ref[...] = jnp.concatenate(demand_rows, axis=1)

    loads[4].wait()
    loads[5].wait()
    for t in range(tiles):
        secs = slice(t * tile_sec, (t + 1) * tile_sec)
        for at in range(0, cap_dev, 128):
            block = jnp.where(survive_v[secs, :, at:at + 128] == 1, mass_v[secs, :, at:at + 128], 0.0)
            place_rows(nat_ref, t, at, block.reshape(128, 128).T)

    loads[6].wait()
    for t in range(tiles):
        secs = slice(t * tile_sec, (t + 1) * tile_sec)
        for at in range(0, cap_dev, 128):
            place_rows(fresh_ref, t, at, start_v[secs, :, at:at + 128].reshape(128, 128).T)

    def weigh(mass, rows, value):
        scrap = 0.3 * col_ref[CAP, rows, :]
        stay = 0.5 + 0.5 * jnp.tanh(value - scrap)
        return mass * stay * col_ref[POW, rows, :]

    def fold_supply(sweep, sums):
        part = jnp.concatenate([one * prod_row for one in sums], axis=0)
        splits = []
        for _ in range(3):
            splits.append(part.astype(jnp.bfloat16).astype(f32))
            part = part - splits[-1]
        grouped = jnp.dot(jnp.concatenate(splits, axis=0).astype(jnp.bfloat16), ones_ref[...],
                          preferred_element_type=f32)
        zsum_ref[...] = grouped[0:tiles * 8] + grouped[tiles * 8:tiles * 16] + grouped[tiles * 16:]
        for t in range(tiles):
            line = zsum_ref[t * 8:t * 8 + 1, :]
            for a in range(1, 8):
                line = line + zsum_ref[t * 8 + a:t * 8 + a + 1, :]
            msg_ref[sweep, :, t * 128:(t + 1) * 128] = line

    def send_supply(sweep, far, close):
        each_other(lambda device: pltpu.make_async_remote_copy(
            src_ref=msg_ref.at[sweep], dst_ref=gat_ref.at[sweep, pl.ds(my_row, 1), :],
            send_sem=msg_send.at[sweep], recv_sem=msg_recv.at[sweep],
            device_id=device, device_id_type=mesh_id).start(), far, close)
        if far:
            gat_ref[sweep, pl.ds(my_row, 1), :] = msg_ref[sweep]

    def wait_rows(count, width, sem):
        view = size_ref.at[pl.ds(0, count), :, pl.ds(0, width)]
        pltpu.make_async_copy(view, view, sem).wait()

    def prices_row(sweep):
        wait_rows(n_dev - 1, lanes + 128, msg_recv.at[sweep])
        every = gat_ref[sweep, 0:n_sec, 0:lanes]
        for c in range(1, n_cap):
            every = every + gat_ref[sweep, c * n_sec:(c + 1) * n_sec, 0:lanes]
        supply = 1.0 + every / (prods * total)
        prices = jnp.sqrt(dems_ref[...] / supply)
        price_ref[...] = prices
        mean = jnp.sum(jnp.sqrt(prices), keepdims=True) / (lanes * n_sec)
        return price_ref[pl.ds(me_sec, 1), :] / (mean * mean)

    def forward():
        halves = []
        for t in range(tiles):
            cont = jnp.maximum(val_ref[t], 0.3 * col_ref[CAP])
            upper = cont.astype(jnp.bfloat16)
            halves.append(jnp.concatenate([upper, (cont - upper.astype(f32)).astype(jnp.bfloat16)], axis=1))
        both = jnp.dot(jnp.concatenate(halves, axis=0), weight_ref[...], preferred_element_type=f32)
        for t in range(tiles):
            runs = [jnp.full((8, 128), NEG, f32)] * (RANGES + 1)
            for at in range(0, cap_dev, 8):
                rows, here = slice(at, at + 8), t * cap_dev + at
                gain = both[here:here + 8, 0:128] + both[here:here + 8, 128:256] + col_ref[GADD, rows, :]
                g_ref[t, rows, :] = gain
                for e in range(RANGES):
                    pre_ref[t, e, rows, :] = runs[e]
                runs = [jnp.maximum(run, gain - qt_ref[e, rows, :]) for e, run in enumerate(runs)]
            for e in range(RANGES + 1):
                ends_ref[t, e] = runs[e]

    def collect(rows_list, rank_rows, count):
        picks = [jnp.full((8, 128), NEG, f32) for _ in range(-(-count // 8))]
        squares = [jnp.zeros((8, 128), f32) for _ in range(-(-count // 8))]
        for (gain, square), rank in zip(rows_list, rank_rows):
            for h in range(-(-count // 8)):
                here = rank == subf + 8.0 * h
                picks[h] = jnp.where(here, gain, picks[h])
                squares[h] = jnp.where(here, square, squares[h])
        return picks, squares

    def prune(sweep, t):
        before, after = bases(ends_ref.at[t], RANGES + 1, sub)

        def down(at, carry):
            runs, counts, gains, squares = carry
            rows = rows_of(steps - 1 - at)
            gain = g_ref[t, rows, :]
            square = col_ref[SQUARE, rows, :]
            points = [gain - qt_ref[e, rows, :] for e in range(RANGES + 1)]
            keep = useful(points[::-1], runs, [pre_ref[t, e, rows, :] for e in range(RANGES)][::-1], before[::-1])
            runs = tuple(jnp.maximum(run, point) for run, point in zip(runs, points[::-1]))
            gains = tuple(jnp.where(keep, new, old) for new, old in zip((gain,) + gains, gains))
            squares = tuple(jnp.where(keep, new, old) for new, old in zip((square,) + squares, squares))
            return runs, counts + jnp.where(keep, 1.0, 0.0), gains, squares

        zero = jnp.zeros((8, 128), f32)
        runs, counts, gains, squares = lax.fori_loop(
            0, steps, down, (tuple(after[::-1]), zero, (zero,) * CHUNK_SLOTS, (zero,) * CHUNK_SLOTS), unroll=8)
        base = counts_before(tot_ref, counts, sub)
        for p in range(CHUNK_SLOTS):
            l1_ref[0, p * 8:(p + 1) * 8, :] = gains[p]
            l1_ref[1, p * 8:(p + 1) * 8, :] = squares[p]
            l1_ref[2, p * 8:(p + 1) * 8, :] = jnp.where(counts > p, base + p, -1.0)
        spots = range(CHUNK_SLOTS * 8)
        picks, squares = collect(
            [(l1_ref[0, r:r + 1, :], l1_ref[1, r:r + 1, :]) for r in spots],
            [l1_ref[2, r:r + 1, :] for r in spots], SLOTS)
        over = flag_row(jnp.where((counts > CHUNK_SLOTS) | (base + counts > SLOTS), 1.0, 0.0))
        for h in range(SLOTS // 8):
            pay_ref[sweep, t, 0, h * 8:(h + 1) * 8, :] = picks[h]
            pay_ref[sweep, t, 1, h * 8:(h + 1) * 8, :] = jnp.where(over > 0.0, -1.0, squares[h])

    def send_payment(sweep, t):
        mine = pl.ds(pl.multiple_of(me_cap * SLOTS, SLOTS), SLOTS)
        for off in range(1, n_cap):
            payment(sweep, t, off).start()
        pays_ref[sweep, t, :, mine, :] = pay_ref[sweep, t]

    def flag_row(flags):
        tot_ref[0] = flags
        return all_max([tot_ref[0, a:a + 1, :] for a in range(8)])

    def payment(sweep, t, off):
        mine = pl.ds(pl.multiple_of(me_cap * SLOTS, SLOTS), SLOTS)
        return pltpu.make_async_remote_copy(
            src_ref=pay_ref.at[sweep, t], dst_ref=pays_ref.at[sweep, t, :, mine, :],
            send_sem=pay_send.at[sweep, t], recv_sem=pay_recv.at[sweep, t],
            device_id={"cap": lax.rem(me_cap + off, n_cap)}, device_id_type=mesh_id)

    def pay_view(sweep, t):
        return pays_ref.at[sweep, t, :, pl.ds(0, (n_cap - 1) * SLOTS), :]

    def merge(sweep, t):
        pltpu.make_async_copy(pay_view(sweep, t), pay_view(sweep, t), pay_recv.at[sweep, t]).wait()
        hops = n_cap * SLOTS // 8

        def line(i):
            spots = pl.ds(i, 8, stride=hops)
            return pays_ref[sweep, t, 0, spots, :], pays_ref[sweep, t, 1, spots, :]

        def back(at, runs):
            i = hops - 1 - at
            gain, square = line(i)
            points = [gain - square * near[e] for e in range(MERGED_RANGES + 1)]
            for e in range(MERGED_RANGES):
                suf_ref[e, rows_of(i), :] = runs[e + 1]
            return tuple(jnp.maximum(run, point) for run, point in zip(runs, points))

        runs = lax.fori_loop(0, hops, back, (jnp.full((8, 128), NEG, f32),) * (MERGED_RANGES + 1), unroll=8)
        for e in range(MERGED_RANGES + 1):
            tot_ref[e] = runs[e]
        before, after = bases(tot_ref, MERGED_RANGES + 1, sub)

        def ahead(i, carry):
            runs, counts, lost = carry
            gain, square = line(i)
            points = [gain - square * near[e] for e in range(MERGED_RANGES + 1)]
            keep = useful(points, runs, [suf_ref[e, rows_of(i), :] for e in range(MERGED_RANGES)], after)
            runs = tuple(jnp.maximum(run, point) for run, point in zip(runs, points))
            pick_ref[0, rows_of(i), :] = jnp.where(keep, counts, NEG)
            return runs, counts + jnp.where(keep, 1.0, 0.0), jnp.minimum(lost, square)

        zero = jnp.zeros((8, 128), f32)
        runs, counts, lost = lax.fori_loop(0, hops, ahead, (tuple(before), zero, zero), unroll=8)
        base = counts_before(tot_ref, counts, sub)
        for i in range(hops):
            pick_ref[0, i * 8:(i + 1) * 8, :] = pick_ref[0, i * 8:(i + 1) * 8, :] + base
        spots = [(i, a) for i in range(hops) for a in range(8)]
        picks, squares = collect(
            [(pays_ref[sweep, t, 0, a * hops + i:a * hops + i + 1, :],
              pays_ref[sweep, t, 1, a * hops + i:a * hops + i + 1, :]) for i, a in spots],
            [pick_ref[0, i * 8 + a:i * 8 + a + 1, :] for i, a in spots], MERGED)
        for h in range(-(-MERGED // 8)):
            pick_ref[1, h * 8:(h + 1) * 8, :] = picks[h]
            pick_ref[2, h * 8:(h + 1) * 8, :] = squares[h]
        return jnp.where(lost < 0.0, 2.0, jnp.where(base + counts > MERGED, 1.0, 0.0))

    def reply(t):
        gains = [jnp.broadcast_to(pick_ref[1, c:c + 1, :], (8, 128)) for c in range(MERGED)]
        squares = [jnp.broadcast_to(pick_ref[2, c:c + 1, :], (8, 128)) for c in range(MERGED)]

        def one(i, carry):
            rows = rows_of(i)
            slope = col_ref[SLOPE, rows, :]
            capital = col_ref[CAP, rows, :]
            moved = all_max([gain - square * slope for gain, square in zip(gains, squares)])
            best_ref[t, rows, :] = jnp.maximum(moved - 1.41 * capital, g_ref[t, rows, :] - 0.91 * capital)
            return carry

        lax.fori_loop(0, steps, one, 0, unroll=8)

    sums = []
    for t in range(tiles):
        def open_step(i, acc, t=t):
            rows = rows_of(i)
            spots = pl.ds(i, 8, stride=pitch)
            mass = jnp.where(exit_rows[t], nat_ref[t, spots, :], 0.0)
            live_ref[t, rows, :] = mass
            value = jnp.where(mass > 0.0, fresh_ref[t, spots, :], 0.3 * col_ref[CAP, rows, :])
            val_ref[t, rows, :] = value
            return acc + weigh(mass, rows, value)

        sums.append(lax.fori_loop(0, steps, open_step, jnp.zeros((8, 128), f32), unroll=16))
    msg_ref[0, :, lanes:lanes + 128] = jnp.zeros((1, 128), f32)
    dem_copies = [pltpu.make_async_remote_copy(
        src_ref=dem_ref, dst_ref=dems_ref.at[pl.ds(me_sec, 1), :], send_sem=dem_send, recv_sem=dem_recv,
        device_id={"sector": lax.rem(me_sec + off, n_sec)}, device_id_type=mesh_id) for off in range(1, n_sec)]
    dems_ref[pl.ds(me_sec, 1), :] = dem_ref[...]
    state = jnp.zeros((8, 128), f32)
    for sweep in range(SWEEPS):
        fold_supply(sweep, sums)
        forward()
        if sweep > 0:
            send_supply(sweep, True, False)
        for t in range(tiles):
            prune(sweep, t)
            if sweep > 0:
                send_payment(sweep, t)
        if sweep == 0:
            pl.semaphore_wait(barrier, n_dev - 1)
            for t in range(tiles):
                send_payment(sweep, t)
            send_supply(sweep, True, False)
            for copy in dem_copies:
                copy.start()
        send_supply(sweep, False, True)
        for t in range(tiles):
            state = jnp.maximum(state, merge(sweep, t))
            reply(t)
        if sweep == 0:
            msg_ref[1, :, lanes:lanes + 128] = flag_row(state)
            state = jnp.zeros((8, 128), f32)
            wait_rows(n_sec - 1, lanes, dem_recv)
        relative = prices_row(sweep)
        if sweep == 0:
            sums = []
            for t in range(tiles):
                scale = relative[:, t * 128:(t + 1) * 128] * prod_row

                def next_step(i, acc, t=t, scale=scale):
                    rows = rows_of(i)
                    mass = live_ref[t, rows, :]
                    value = jnp.where(mass > 0.0,
                                      scale * col_ref[POW, rows, :] + best_ref[t, rows, :],
                                      0.3 * col_ref[CAP, rows, :])
                    val_ref[t, rows, :] = value
                    return acc + weigh(mass, rows, value)

                sums.append(lax.fori_loop(0, steps, next_step, jnp.zeros((8, 128), f32), unroll=16))
    rel_ref[...] = relative
    early = jnp.max(gat_ref[1, :, lanes:lanes + 128], axis=0, keepdims=True)
    flag_ref[0] = jnp.max(jnp.maximum(state, jnp.where(early > 0.0, 3.0, 0.0))).astype(jnp.int32)
    report = pltpu.make_async_copy(flag_ref, flag_hbm, in_sem.at[0])
    report.start()
    for t in range(tiles):
        scale = relative[:, t * 128:(t + 1) * 128] * prod_row

        def last_step(i, carry, t=t, scale=scale):
            rows = rows_of(i)
            out_ref[t, pl.ds(i, 8, stride=pitch), :] = jnp.where(
                live_ref[t, rows, :] > 0.0, scale * col_ref[POW, rows, :] + best_ref[t, rows, :],
                0.3 * col_ref[CAP, rows, :])
            return carry

        lax.fori_loop(0, steps, last_step, 0, unroll=8)
    cand_ref[...] = pays_ref[SWEEPS - 1]
    for sweep in range(SWEEPS):
        wait_rows(n_dev - 1, lanes + 128, msg_send.at[sweep])
        for t in range(tiles):
            pltpu.make_async_copy(pay_view(sweep, t), pay_view(sweep, t), pay_send.at[sweep, t]).wait()
    wait_rows(n_sec - 1, lanes, dem_send)
    report.wait()


def pruned_sweeps(start_value, firm_mass, survive, exit_index, demand, transition, install_cost):
    n_sec, n_cap = lax.axis_size("sector"), lax.axis_size("cap")
    sec_dev, prods, cap_dev = start_value.shape
    lanes = sec_dev * prods
    tiles = lanes // 128
    n_dev = n_sec * n_cap
    far = pl.BlockSpec(memory_space=pl.ANY)
    vmem = pl.BlockSpec(memory_space=pltpu.VMEM)
    smem = pl.BlockSpec(memory_space=pltpu.SMEM)
    f32 = jnp.float32
    dma = pltpu.SemaphoreType.DMA
    pack = max(RANGES, MERGED_RANGES)
    return pl.pallas_call(
        functools.partial(sweeps_kernel, n_sec, n_cap),
        out_shape=(
            jax.ShapeDtypeStruct((tiles, cap_dev + 64, 128), f32),
            jax.ShapeDtypeStruct((tiles, cap_dev, 128), f32),
            jax.ShapeDtypeStruct((tiles, 2, n_cap * SLOTS, 128), f32),
            jax.ShapeDtypeStruct((1, lanes), f32),
            jax.ShapeDtypeStruct((1,), jnp.int32),
        ),
        in_specs=[far] * 7,
        out_specs=(vmem, vmem, vmem, vmem, far),
        scratch_shapes=[
            pltpu.VMEM(start_value.shape, f32),
            pltpu.VMEM(start_value.shape, f32),
            pltpu.VMEM(start_value.shape, jnp.int32),
            pltpu.SMEM((sec_dev,), jnp.int32),
            pltpu.SMEM((sec_dev,), f32),
            pltpu.VMEM((prods, prods), f32),
            pltpu.VMEM((1, cap_dev), f32),
            pltpu.VMEM((tiles, cap_dev + 64, 128), f32),
            pltpu.VMEM((tiles, cap_dev + 64, 128), f32),
            pltpu.VMEM((tiles, cap_dev, 128), f32),
            pltpu.VMEM((tiles, cap_dev, 128), f32),
            pltpu.VMEM((tiles, RANGES, cap_dev, 128), f32),
            pltpu.VMEM((tiles, RANGES + 1, 8, 128), f32),
            pltpu.VMEM((MERGED_RANGES, n_cap * SLOTS, 128), f32),
            pltpu.VMEM((tiles, cap_dev, 128), f32),
            pltpu.VMEM((5, cap_dev, 128), f32),
            pltpu.VMEM((RANGES + 1, cap_dev, 128), f32),
            pltpu.VMEM((256, 256), jnp.bfloat16),
            pltpu.VMEM((128, 128), jnp.bfloat16),
            pltpu.VMEM((pack + 1, 8, 128), f32),
            pltpu.VMEM((3, CHUNK_SLOTS * 8, 128), f32),
            pltpu.VMEM((3, max(MERGED, n_cap * SLOTS), 128), f32),
            pltpu.VMEM((tiles * 8, 128), f32),
            pltpu.VMEM((n_sec, lanes), f32),
            pltpu.VMEM((SWEEPS, 1, lanes + 128), f32),
            pltpu.VMEM((SWEEPS, n_dev, lanes + 128), f32),
            pltpu.VMEM((1, lanes), f32),
            pltpu.VMEM((n_sec, lanes), f32),
            pltpu.VMEM((SWEEPS, tiles, 2, SLOTS, 128), f32),
            pltpu.VMEM((SWEEPS, tiles, 2, n_cap * SLOTS, 128), f32),
            pltpu.VMEM((n_dev - 1, 1, lanes + 128), f32),
            pltpu.SMEM((1,), jnp.int32),
            dma((7,)),
            dma((SWEEPS,)), dma((SWEEPS,)), dma, dma,
            dma((SWEEPS, tiles)), dma((SWEEPS, tiles)),
        ],
        compiler_params=pltpu.CompilerParams(
            collective_id=0, has_side_effects=True, vmem_limit_bytes=48 * 1024 * 1024
        ),
    )(start_value, firm_mass, survive, exit_index, demand, transition, install_cost[None, :])


def all_candidates(values, candidates, relative, survive, exit_index):
    sec_dev, prods, cap_dev = values.shape
    total = cap_dev * lax.axis_size("cap")
    capital = capital_of(lax.axis_index("cap") * cap_dev + jnp.arange(cap_dev, dtype=jnp.int32), total)
    prod_index = jnp.arange(prods, dtype=jnp.int32)
    output = jnp.exp(-0.5 + prod_index.astype(jnp.float32) / (prods - 1))[:, None] * capital[None, :] ** 0.6
    live = (survive == 1) & (prod_index[None, :, None] >= exit_index[:, None, None])
    flat = jnp.moveaxis(candidates, 0, 2).reshape(2, candidates.shape[2], sec_dev, prods)

    def one(best, pair):
        return jnp.maximum(best, pair[0][:, :, None] - pair[1][:, :, None] / capital), None

    moved, _ = lax.scan(one, jnp.full(values.shape, NEG, jnp.float32), (flat[0], flat[1]))
    again = relative[:, None, None] * output + (moved - 1.41 * capital)
    return jnp.where(live, jnp.maximum(values, again), values)


def group_sweep(gains, relative, survive, exit_index):
    sec_dev, prods, cap_dev = survive.shape
    tiles = gains.shape[0]
    total = cap_dev * lax.axis_size("cap")
    row_first = lax.axis_index("cap") * cap_dev
    capital = capital_of(row_first + jnp.arange(cap_dev, dtype=jnp.int32), total)
    prod_index = jnp.arange(prods, dtype=jnp.int32)
    output = jnp.exp(-0.5 + prod_index.astype(jnp.float32) / (prods - 1))[:, None] * capital[None, :] ** 0.6
    live = (survive == 1) & (prod_index[None, :, None] >= exit_index[:, None, None])
    natural = gains.reshape(tiles, cap_dev // 8, 8, 128).swapaxes(1, 2).reshape(tiles, cap_dev, 128)
    forward_value = natural.swapaxes(1, 2).reshape(sec_dev, prods, cap_dev) - 0.8 * capital
    rows = jnp.moveaxis(gather_blocks(forward_value, "cap"), 0, 2).reshape(sec_dev * prods, total)
    best = best_reply(rows, row_first, cap_dev).reshape(sec_dev, prods, cap_dev)
    return jnp.where(live, relative[:, None, None] * output + best, 0.3 * capital)


def finish_kernel(flipped_ref, row_ref, out_ref, rel_ref):
    tile_sec, prods, cap_dev = out_ref.shape
    lanes, sec_dev = row_ref.shape[1], rel_ref.shape[1]
    steps = cap_dev // 8
    for at in range(0, cap_dev, 128):
        spots = [(at + up) // steps * (steps + 8) for up in range(0, 128, steps)]
        block = jnp.concatenate([flipped_ref[0, spot:spot + steps, :] for spot in spots], axis=0)
        out_ref[:, :, at:at + 128] = block.T.reshape(tile_sec, prods, 128)

    @pl.when(pl.program_id(0) == 0)
    def _():
        column = jnp.sum(jnp.where(
            lax.broadcasted_iota(jnp.int32, (sec_dev, lanes), 1) == prods * lax.broadcasted_iota(
                jnp.int32, (sec_dev, lanes), 0), row_ref[...], 0.0), axis=1, keepdims=True)
        spot = lax.broadcasted_iota(jnp.int32, (sec_dev, sec_dev), 0) == lax.broadcasted_iota(
            jnp.int32, (sec_dev, sec_dev), 1)
        rel_ref[...] = jnp.sum(jnp.where(spot, column, 0.0), axis=0, keepdims=True)


def finish(flipped, row, sec_dev, prods):
    tiles, padded, _ = flipped.shape
    cap_dev = padded - 64
    values, relative = pl.pallas_call(
        finish_kernel,
        grid=(tiles,),
        out_shape=(jax.ShapeDtypeStruct((sec_dev, prods, cap_dev), jnp.float32),
                   jax.ShapeDtypeStruct((1, sec_dev), jnp.float32)),
        in_specs=[pl.BlockSpec((1, padded, 128), lambda t: (t, 0, 0)),
                  pl.BlockSpec(row.shape, lambda t: (0, 0))],
        out_specs=(pl.BlockSpec((sec_dev // tiles, prods, cap_dev), lambda t: (t, 0, 0)),
                   pl.BlockSpec((1, sec_dev), lambda t: (0, 0))),
    )(flipped, row)
    return values, relative[0]


def on_device(start_value, firm_mass, survive, exit_index, demand, transition, install_cost):
    args = (start_value, firm_mass, survive, exit_index, demand, transition, install_cost)
    sec_dev, prods, cap_dev = start_value.shape
    if 128 % prods or prods % 8 or sec_dev * prods % 128 or cap_dev % 128 or min(
            lax.axis_size("sector"), lax.axis_size("cap")) < 2:
        return dense_sweeps(*args)
    flipped, gains, candidates, row, state = pruned_sweeps(*args)

    def plain():
        return finish(flipped, row, sec_dev, prods)

    def wide():
        values, relative = plain()
        return all_candidates(values, candidates, relative, survive, exit_index), relative

    def group():
        relative = row.reshape(sec_dev, prods)[:, 0]
        return group_sweep(gains, relative, survive, exit_index), relative

    return lax.switch(state[0], (plain, wide, group, lambda: dense_sweeps(*args)))


def solution(mesh):
    return jax.shard_map(
        on_device,
        mesh=mesh,
        in_specs=(
            P("sector", None, "cap"),
            P("sector", None, "cap"),
            P("sector", None, "cap"),
            P("sector"),
            P("sector"),
            P(),
            P("cap"),
        ),
        out_specs=(P("sector", None, "cap"), P("sector")),
        check_vma=False,
    )
```

```python
import functools
import math

import jax
import jax.numpy as jnp
from jax import lax
from jax.experimental import pallas as pl
from jax.experimental.pallas import tpu as pltpu
from jax.sharding import PartitionSpec as P

SWEEPS = 2
CHUNK_SLOTS = 8
SLOTS = 16
MERGED = 12
UNROLLED_DEVICES = 64
RANGES = 4
MERGED_RANGES = 2
NEG = -1e30
LOG_TEN = math.log(10.0)


def capital_of(positions, total):
    return 0.2 * jnp.exp(LOG_TEN * positions.astype(jnp.float32) / (total - 1))


def charge_of(cap_now, cap_next, row_ids, col_ids):
    invest = cap_next - 0.9 * cap_now
    fixed = jnp.where(row_ids == col_ids, 0.0, 1.5 * cap_now)
    return invest + invest * invest / cap_now + fixed


def best_reply(forward_rows, row_first, row_count):
    total_rows, total_cols = forward_rows.shape
    cap_of = functools.partial(capital_of, total=total_cols)
    col_block = math.gcd(total_cols, 2048)
    row_block = math.gcd(row_count, 512)
    grp_limit = max(1, (1 << 24) // (row_block * col_block))
    grp_size = math.gcd(total_rows, 1 << min(total_rows, grp_limit).bit_length() - 1)
    groups = forward_rows.reshape(total_rows // grp_size, grp_size, total_cols)

    def one_group(group):
        row_ids = row_first + jnp.arange(row_count, dtype=jnp.int32)
        cap_rows = cap_of(row_ids)
        col_ids = jnp.arange(total_cols, dtype=jnp.int32)
        cap_cols = cap_of(col_ids)
        charge = charge_of(cap_rows[:, None], cap_cols[None, :], row_ids[:, None], col_ids[None, :])
        return jnp.max(group[:, None, :] - charge[None], axis=2)

    return lax.map(one_group, groups).reshape(total_rows, row_count)


def gather_blocks(block, axis_name):
    count = lax.axis_size(axis_name)
    me = lax.axis_index(axis_name)
    parts = [block]
    for off in range(1, count):
        parts.append(lax.ppermute(block, axis_name, [(d, (d + off) % count) for d in range(count)]))
    return jnp.take(jnp.stack(parts), (me - jnp.arange(count) + count) % count, axis=0)


def dense_sweeps(start_value, firm_mass, survive, exit_index, demand, transition, install_cost):
    sec_dev, prod_count, cap_dev = start_value.shape
    sectors_all = sec_dev * lax.axis_size("sector")
    row_first = lax.axis_index("cap") * cap_dev
    prod_index = jnp.arange(prod_count, dtype=jnp.int32)
    total = cap_dev * lax.axis_size("cap")
    capital = capital_of(row_first + jnp.arange(cap_dev, dtype=jnp.int32), total)
    log_prod = -0.5 + prod_index.astype(jnp.float32) / (prod_count - 1)
    output = jnp.exp(log_prod)[:, None] * capital[None, :] ** 0.6
    scrap = 0.3 * capital
    live = (survive == 1) & (prod_index[None, :, None] >= exit_index[:, None, None])
    values = start_value
    relative = jnp.zeros((sec_dev,), jnp.float32)
    for sweep in range(SWEEPS):
        staying = jnp.where(live, jax.nn.sigmoid((values - scrap) / 0.5), 0.0)
        partial_value = jnp.sum(firm_mass * staying * output, axis=(1, 2))
        supply = 1.0 + jnp.sum(gather_blocks(partial_value, "cap"), axis=0) / (prod_count * total)
        prices = jnp.sqrt(demand / supply)
        root_sum = jnp.sum(gather_blocks(jnp.sqrt(prices), "sector"))
        price_index = (root_sum / sectors_all) ** 2
        relative = prices / price_index
        continuation = jnp.where(live, jnp.maximum(values, scrap), scrap)
        expect = jnp.einsum(
            "zw,swk->szk", transition, continuation, precision=lax.Precision.HIGHEST
        )
        forward_value = 0.9 * expect - install_cost[None, None, :]
        blocks = gather_blocks(forward_value, "cap")
        rows = jnp.moveaxis(blocks, 0, 2).reshape(sec_dev * prod_count, total)
        best = best_reply(rows, row_first, cap_dev).reshape(sec_dev, prod_count, cap_dev)
        values = jnp.where(live, relative[:, None, None] * output + best, scrap)
    return (values, relative)


def rows_of(step):
    return pl.ds(pl.multiple_of(step * 8, 8), 8)


def all_max(parts):
    return functools.reduce(jnp.maximum, parts)


def bases(tot_ref, count, sub):
    before, after = [], []
    for e in range(count):
        rows = [tot_ref[e, a:a + 1, :] for a in range(8)]
        if e < count - 1:
            before.append(all_max([jnp.where(sub > a, rows[a], NEG) for a in range(7)]))
        if e > 0:
            after.append(all_max([jnp.where(sub < a, rows[a], NEG) for a in range(1, 8)]))
    return before, after


def counts_before(tot_ref, counts, sub):
    tot_ref[0] = counts
    base = jnp.zeros_like(counts)
    for a in range(7):
        base = base + jnp.where(sub > a, tot_ref[0, a:a + 1, :], 0.0)
    return base


def useful(points, runs, sufs, afters):
    keep = None
    for e in range(len(runs)):
        good = (points[e] > runs[e]) & (points[e + 1] > jnp.maximum(sufs[e], afters[e]))
        keep = good if keep is None else keep | good
    return keep


def sweeps_kernel(n_sec, n_cap, start_hbm, mass_hbm, survive_hbm, exit_hbm, demand_hbm, trans_hbm, cost_hbm,
                  out_ref, g_ref, cand_ref, rel_ref, flag_hbm,
                  start_v, mass_v, survive_v, exit_v, demand_v, trans_v, cost_v,
                  nat_ref, fresh_ref, val_ref, live_ref, pre_ref, ends_ref, suf_ref, best_ref, col_ref, qt_ref,
                  weight_ref, ones_ref, tot_ref, l1_ref, pick_ref, zsum_ref, price_ref,
                  msg_ref, gat_ref, dem_ref, dems_ref, pay_ref, pays_ref, size_ref, flag_ref,
                  in_sem, msg_send, msg_recv, dem_send, dem_recv, pay_send, pay_recv):
    sec_dev, prods, cap_dev = start_v.shape
    total = cap_dev * n_cap
    steps = cap_dev // 8
    pitch = steps + 8
    tiles = sec_dev * prods // 128
    tile_sec = 128 // prods
    lanes = tiles * 128
    col_tiles = cap_dev // 128
    n_dev = n_sec * n_cap
    me_cap = lax.axis_index("cap")
    me_sec = lax.axis_index("sector")
    me = me_sec * n_cap + me_cap
    my_row = me_cap * n_sec + me_sec
    mesh_id = pl.DeviceIdType.MESH
    f32 = jnp.float32

    def each_other(act, far=True, close=True):
        if n_dev > UNROLLED_DEVICES:
            if not far:
                return

            def one(off, carry):
                index = lax.rem(me + off, n_dev)
                act({"sector": index // n_cap, "cap": lax.rem(index, n_cap)})
                return carry

            lax.fori_loop(1, n_dev, one, 0)
            return
        upper = me_sec * 2 // n_sec
        skip = me_sec + upper * (n_sec - 1 - 2 * me_sec)
        for j in range(0 if far else n_sec // 2, n_sec - 1 if close else n_sec // 2):
            spot = n_sec - 1 - j - (j + 1 + skip) // n_sec
            other = spot + upper * (n_sec - 1 - 2 * spot)
            for c in range(n_cap):
                act({"sector": other, "cap": lax.rem(me_cap + c, n_cap)})
        for c in range(1, n_cap if close else 1):
            act({"sector": me_sec, "cap": lax.rem(me_cap + c, n_cap)})

    loads = []
    for at, (src, dst) in enumerate((
        (trans_hbm, trans_v), (cost_hbm, cost_v), (exit_hbm, exit_v), (demand_hbm, demand_v),
        (mass_hbm, mass_v), (survive_hbm, survive_v), (start_hbm, start_v),
    )):
        loads.append(pltpu.make_async_copy(src, dst, in_sem.at[at]))
        loads[-1].start()

    barrier = pltpu.get_barrier_semaphore()
    each_other(lambda device: pl.semaphore_signal(barrier, inc=1, device_id=device, device_id_type=mesh_id))
    sub = lax.broadcasted_iota(jnp.int32, (8, 128), 0)
    subf = sub.astype(f32)
    lane = lax.broadcasted_iota(jnp.int32, (1, 128), 1)
    lane_prod = lax.rem(lane, prods)
    lane_sec = lane // prods
    ends = [0.5 * 10.0 ** (e / RANGES) for e in range(RANGES + 1)]
    ends[0] *= 1.0 - 1e-5
    ends[-1] *= 1.0 + 1e-5
    first = me_cap * cap_dev
    CAP, SLOPE, POW, GADD, SQUARE = range(5)

    row = lax.broadcasted_iota(jnp.int32, (cap_dev, 128), 0)
    place = first + lax.rem(row, 8) * steps + row // 8
    capital = capital_of(place, total)
    col_ref[CAP] = capital
    col_ref[SLOPE] = 1.0 / capital
    col_ref[POW] = jnp.exp(0.6 * (math.log(0.2) + LOG_TEN * place.astype(f32) / (total - 1)))
    col_ref[SQUARE] = capital * capital
    for e in range(RANGES + 1):
        qt_ref[e] = capital * capital * ends[e]
    edge = [first + cap_dev - 1, first]
    t_low, t_high = [1.0 / capital_of(jnp.full((8, 128), at, jnp.int32), total) for at in edge]
    t_low, t_high = t_low * (1.0 - 1e-5), t_high * (1.0 + 1e-5)
    log_low, log_high = jnp.log(t_low), jnp.log(t_high)
    near = [t_low] + [
        jnp.exp(log_low + (log_high - log_low) * (e / MERGED_RANGES)) for e in range(1, MERGED_RANGES)
    ] + [t_high]
    prod_row = jnp.exp(-0.5 + lane_prod.astype(f32) / (prods - 1))
    big_r = lax.broadcasted_iota(jnp.int32, (128, 128), 0)
    big_c = lax.broadcasted_iota(jnp.int32, (128, 128), 1)
    same = big_r // prods == big_c // prods
    ones_ref[...] = jnp.where(same, 1.0, 0.0).astype(jnp.bfloat16)

    loads[0].wait()
    spot_r = lax.broadcasted_iota(jnp.int32, (128, prods), 0)
    spot_c = lax.broadcasted_iota(jnp.int32, (128, prods), 1)
    spot = jnp.where(lax.rem(spot_r, prods) == spot_c, 1.0, 0.0).astype(jnp.bfloat16)
    scaled = 0.9 * trans_v[...]
    upper = scaled.astype(jnp.bfloat16)
    pair = jnp.concatenate([upper, (scaled - upper.astype(f32)).astype(jnp.bfloat16)], axis=0)
    half = lax.dot_general(spot, pair, (((1,), (1,)), ((), ())), preferred_element_type=f32)
    fan_r = lax.broadcasted_iota(jnp.int32, (2 * prods, 256), 0)
    fan_c = lax.broadcasted_iota(jnp.int32, (2 * prods, 256), 1)
    fan = (lax.rem(fan_r, prods) == lax.rem(fan_c, prods)) & (fan_r // prods == fan_c // 128)
    full = jnp.dot(half.astype(jnp.bfloat16), jnp.where(fan, 1.0, 0.0).astype(jnp.bfloat16), preferred_element_type=f32)
    top = jnp.where(same, full[:, 0:128], 0.0).astype(jnp.bfloat16)
    low = jnp.where(same, full[:, 128:256], 0.0).astype(jnp.bfloat16)
    weight_ref[0:128, 0:128] = top
    weight_ref[128:256, 0:128] = top
    weight_ref[0:128, 128:256] = low
    weight_ref[128:256, 128:256] = jnp.zeros_like(low)

    def place_rows(ref, t, at, block):
        for up in range(0, 128, steps):
            spot = (at + up) // steps * pitch
            ref[t, spot:spot + steps, :] = block[up:up + steps]

    loads[1].wait()
    for at in range(0, cap_dev, 128):
        place_rows(nat_ref, 0, at, jnp.broadcast_to(cost_v[:, at:at + 128], (128, 128)).T)

    def add_step(i, carry):
        rows = rows_of(i)
        col_ref[GADD, rows, :] = 0.8 * col_ref[CAP, rows, :] - nat_ref[0, pl.ds(i, 8, stride=pitch), :]
        return carry

    lax.fori_loop(0, steps, add_step, 0, unroll=8)

    loads[2].wait()
    loads[3].wait()
    exit_rows, demand_rows = [], []
    for t in range(tiles):
        exit_row = jnp.zeros((1, 128), jnp.int32)
        demand_row = jnp.zeros((1, 128), f32)
        for s in range(tile_sec):
            exit_row = jnp.where(lane_sec == s, exit_v[t * tile_sec + s], exit_row)
            demand_row = jnp.where(lane_sec == s, demand_v[t * tile_sec + s], demand_row)
        exit_rows.append(lane_prod >= exit_row)
        demand_rows.append(demand_row)
    dem_ref[...] = jnp.concatenate(demand_rows, axis=1)

    loads[4].wait()
    loads[5].wait()
    for t in range(tiles):
        secs = slice(t * tile_sec, (t + 1) * tile_sec)
        for at in range(0, cap_dev, 128):
            block = jnp.where(survive_v[secs, :, at:at + 128] == 1, mass_v[secs, :, at:at + 128], 0.0)
            place_rows(nat_ref, t, at, block.reshape(128, 128).T)

    loads[6].wait()
    for t in range(tiles):
        secs = slice(t * tile_sec, (t + 1) * tile_sec)
        for at in range(0, cap_dev, 128):
            place_rows(fresh_ref, t, at, start_v[secs, :, at:at + 128].reshape(128, 128).T)

    def weigh(mass, rows, value):
        scrap = 0.3 * col_ref[CAP, rows, :]
        stay = 0.5 + 0.5 * jnp.tanh(value - scrap)
        return mass * stay * col_ref[POW, rows, :]

    def fold_supply(sweep, sums):
        part = jnp.concatenate([one * prod_row for one in sums], axis=0)
        splits = []
        for _ in range(3):
            splits.append(part.astype(jnp.bfloat16).astype(f32))
            part = part - splits[-1]
        grouped = jnp.dot(jnp.concatenate(splits, axis=0).astype(jnp.bfloat16), ones_ref[...],
                          preferred_element_type=f32)
        zsum_ref[...] = grouped[0:tiles * 8] + grouped[tiles * 8:tiles * 16] + grouped[tiles * 16:]
        for t in range(tiles):
            line = zsum_ref[t * 8:t * 8 + 1, :]
            for a in range(1, 8):
                line = line + zsum_ref[t * 8 + a:t * 8 + a + 1, :]
            msg_ref[sweep, :, t * 128:(t + 1) * 128] = line

    def send_supply(sweep, far, close):
        each_other(lambda device: pltpu.make_async_remote_copy(
            src_ref=msg_ref.at[sweep], dst_ref=gat_ref.at[sweep, pl.ds(my_row, 1), :],
            send_sem=msg_send.at[sweep], recv_sem=msg_recv.at[sweep],
            device_id=device, device_id_type=mesh_id).start(), far, close)
        if far:
            gat_ref[sweep, pl.ds(my_row, 1), :] = msg_ref[sweep]

    def wait_rows(count, width, sem):
        view = size_ref.at[pl.ds(0, count), :, pl.ds(0, width)]
        pltpu.make_async_copy(view, view, sem).wait()

    def prices_row(sweep):
        wait_rows(n_dev - 1, lanes + 128, msg_recv.at[sweep])
        every = gat_ref[sweep, 0:n_sec, 0:lanes]
        for c in range(1, n_cap):
            every = every + gat_ref[sweep, c * n_sec:(c + 1) * n_sec, 0:lanes]
        supply = 1.0 + every / (prods * total)
        prices = jnp.sqrt(dems_ref[...] / supply)
        price_ref[...] = prices
        mean = jnp.sum(jnp.sqrt(prices), keepdims=True) / (lanes * n_sec)
        return price_ref[pl.ds(me_sec, 1), :] / (mean * mean)

    def forward():
        halves = []
        for t in range(tiles):
            cont = jnp.maximum(val_ref[t], 0.3 * col_ref[CAP])
            upper = cont.astype(jnp.bfloat16)
            halves.append(jnp.concatenate([upper, (cont - upper.astype(f32)).astype(jnp.bfloat16)], axis=1))
        both = jnp.dot(jnp.concatenate(halves, axis=0), weight_ref[...], preferred_element_type=f32)
        for t in range(tiles):
            runs = [jnp.full((8, 128), NEG, f32)] * (RANGES + 1)
            for at in range(0, cap_dev, 8):
                rows, here = slice(at, at + 8), t * cap_dev + at
                gain = both[here:here + 8, 0:128] + both[here:here + 8, 128:256] + col_ref[GADD, rows, :]
                g_ref[t, rows, :] = gain
                for e in range(RANGES):
                    pre_ref[t, e, rows, :] = runs[e]
                runs = [jnp.maximum(run, gain - qt_ref[e, rows, :]) for e, run in enumerate(runs)]
            for e in range(RANGES + 1):
                ends_ref[t, e] = runs[e]

    def collect(rows_list, rank_rows, count):
        picks = [jnp.full((8, 128), NEG, f32) for _ in range(-(-count // 8))]
        squares = [jnp.zeros((8, 128), f32) for _ in range(-(-count // 8))]
        for (gain, square), rank in zip(rows_list, rank_rows):
            for h in range(-(-count // 8)):
                here = rank == subf + 8.0 * h
                picks[h] = jnp.where(here, gain, picks[h])
                squares[h] = jnp.where(here, square, squares[h])
        return picks, squares

    def prune(sweep, t):
        before, after = bases(ends_ref.at[t], RANGES + 1, sub)

        def down(at, carry):
            runs, counts, gains, squares = carry
            rows = rows_of(steps - 1 - at)
            gain = g_ref[t, rows, :]
            square = col_ref[SQUARE, rows, :]
            points = [gain - qt_ref[e, rows, :] for e in range(RANGES + 1)]
            keep = useful(points[::-1], runs, [pre_ref[t, e, rows, :] for e in range(RANGES)][::-1], before[::-1])
            runs = tuple(jnp.maximum(run, point) for run, point in zip(runs, points[::-1]))
            gains = tuple(jnp.where(keep, new, old) for new, old in zip((gain,) + gains, gains))
            squares = tuple(jnp.where(keep, new, old) for new, old in zip((square,) + squares, squares))
            return runs, counts + jnp.where(keep, 1.0, 0.0), gains, squares

        zero = jnp.zeros((8, 128), f32)
        runs, counts, gains, squares = lax.fori_loop(
            0, steps, down, (tuple(after[::-1]), zero, (zero,) * CHUNK_SLOTS, (zero,) * CHUNK_SLOTS), unroll=16)
        base = counts_before(tot_ref, counts, sub)
        for p in range(CHUNK_SLOTS):
            l1_ref[0, p * 8:(p + 1) * 8, :] = gains[p]
            l1_ref[1, p * 8:(p + 1) * 8, :] = squares[p]
            l1_ref[2, p * 8:(p + 1) * 8, :] = jnp.where(counts > p, base + p, -1.0)
        spots = range(CHUNK_SLOTS * 8)
        picks, squares = collect(
            [(l1_ref[0, r:r + 1, :], l1_ref[1, r:r + 1, :]) for r in spots],
            [l1_ref[2, r:r + 1, :] for r in spots], SLOTS)
        over = flag_row(jnp.where((counts > CHUNK_SLOTS) | (base + counts > SLOTS), 1.0, 0.0))
        for h in range(SLOTS // 8):
            pay_ref[sweep, t, 0, h * 8:(h + 1) * 8, :] = picks[h]
            pay_ref[sweep, t, 1, h * 8:(h + 1) * 8, :] = jnp.where(over > 0.0, -1.0, squares[h])

    def send_payment(sweep, t):
        mine = pl.ds(pl.multiple_of(me_cap * SLOTS, SLOTS), SLOTS)
        for off in range(1, n_cap):
            payment(sweep, t, off).start()
        pays_ref[sweep, t, :, mine, :] = pay_ref[sweep, t]

    def flag_row(flags):
        tot_ref[0] = flags
        return all_max([tot_ref[0, a:a + 1, :] for a in range(8)])

    def payment(sweep, t, off):
        mine = pl.ds(pl.multiple_of(me_cap * SLOTS, SLOTS), SLOTS)
        return pltpu.make_async_remote_copy(
            src_ref=pay_ref.at[sweep, t], dst_ref=pays_ref.at[sweep, t, :, mine, :],
            send_sem=pay_send.at[sweep, t], recv_sem=pay_recv.at[sweep, t],
            device_id={"cap": lax.rem(me_cap + off, n_cap)}, device_id_type=mesh_id)

    def pay_view(sweep, t):
        return pays_ref.at[sweep, t, :, pl.ds(0, (n_cap - 1) * SLOTS), :]

    def merge(sweep, t):
        pltpu.make_async_copy(pay_view(sweep, t), pay_view(sweep, t), pay_recv.at[sweep, t]).wait()
        hops = n_cap * SLOTS // 8

        def line(i):
            spots = pl.ds(i, 8, stride=hops)
            return pays_ref[sweep, t, 0, spots, :], pays_ref[sweep, t, 1, spots, :]

        def back(at, runs):
            i = hops - 1 - at
            gain, square = line(i)
            points = [gain - square * near[e] for e in range(MERGED_RANGES + 1)]
            for e in range(MERGED_RANGES):
                suf_ref[e, rows_of(i), :] = runs[e + 1]
            return tuple(jnp.maximum(run, point) for run, point in zip(runs, points))

        runs = lax.fori_loop(0, hops, back, (jnp.full((8, 128), NEG, f32),) * (MERGED_RANGES + 1), unroll=8)
        for e in range(MERGED_RANGES + 1):
            tot_ref[e] = runs[e]
        before, after = bases(tot_ref, MERGED_RANGES + 1, sub)

        def ahead(i, carry):
            runs, counts, lost = carry
            gain, square = line(i)
            points = [gain - square * near[e] for e in range(MERGED_RANGES + 1)]
            keep = useful(points, runs, [suf_ref[e, rows_of(i), :] for e in range(MERGED_RANGES)], after)
            runs = tuple(jnp.maximum(run, point) for run, point in zip(runs, points))
            pick_ref[0, rows_of(i), :] = jnp.where(keep, counts, NEG)
            return runs, counts + jnp.where(keep, 1.0, 0.0), jnp.minimum(lost, square)

        zero = jnp.zeros((8, 128), f32)
        runs, counts, lost = lax.fori_loop(0, hops, ahead, (tuple(before), zero, zero), unroll=8)
        base = counts_before(tot_ref, counts, sub)
        for i in range(hops):
            pick_ref[0, i * 8:(i + 1) * 8, :] = pick_ref[0, i * 8:(i + 1) * 8, :] + base
        spots = [(i, a) for i in range(hops) for a in range(8)]
        picks, squares = collect(
            [(pays_ref[sweep, t, 0, a * hops + i:a * hops + i + 1, :],
              pays_ref[sweep, t, 1, a * hops + i:a * hops + i + 1, :]) for i, a in spots],
            [pick_ref[0, i * 8 + a:i * 8 + a + 1, :] for i, a in spots], MERGED)
        for h in range(-(-MERGED // 8)):
            pick_ref[1, h * 8:(h + 1) * 8, :] = picks[h]
            pick_ref[2, h * 8:(h + 1) * 8, :] = squares[h]
        return jnp.where(lost < 0.0, 2.0, jnp.where(base + counts > MERGED, 1.0, 0.0))

    def reply(t):
        gains = [jnp.broadcast_to(pick_ref[1, c:c + 1, :], (8, 128)) for c in range(MERGED)]
        squares = [jnp.broadcast_to(pick_ref[2, c:c + 1, :], (8, 128)) for c in range(MERGED)]

        def one(i, carry):
            rows = rows_of(i)
            slope = col_ref[SLOPE, rows, :]
            capital = col_ref[CAP, rows, :]
            moved = all_max([gain - square * slope for gain, square in zip(gains, squares)])
            best_ref[t, rows, :] = jnp.maximum(moved - 1.41 * capital, g_ref[t, rows, :] - 0.91 * capital)
            return carry

        lax.fori_loop(0, steps, one, 0, unroll=16)

    sums = []
    for t in range(tiles):
        def open_step(i, acc, t=t):
            rows = rows_of(i)
            spots = pl.ds(i, 8, stride=pitch)
            mass = jnp.where(exit_rows[t], nat_ref[t, spots, :], 0.0)
            live_ref[t, rows, :] = mass
            value = jnp.where(mass > 0.0, fresh_ref[t, spots, :], 0.3 * col_ref[CAP, rows, :])
            val_ref[t, rows, :] = value
            return acc + weigh(mass, rows, value)

        sums.append(lax.fori_loop(0, steps, open_step, jnp.zeros((8, 128), f32), unroll=16))
    msg_ref[0, :, lanes:lanes + 128] = jnp.zeros((1, 128), f32)
    dem_copies = [pltpu.make_async_remote_copy(
        src_ref=dem_ref, dst_ref=dems_ref.at[pl.ds(me_sec, 1), :], send_sem=dem_send, recv_sem=dem_recv,
        device_id={"sector": lax.rem(me_sec + off, n_sec)}, device_id_type=mesh_id) for off in range(1, n_sec)]
    dems_ref[pl.ds(me_sec, 1), :] = dem_ref[...]
    state = jnp.zeros((8, 128), f32)
    for sweep in range(SWEEPS):
        fold_supply(sweep, sums)
        forward()
        if sweep > 0:
            send_supply(sweep, True, False)
        for t in range(tiles):
            prune(sweep, t)
            if sweep > 0:
                send_payment(sweep, t)
        if sweep == 0:
            pl.semaphore_wait(barrier, n_dev - 1)
            for t in range(tiles):
                send_payment(sweep, t)
            send_supply(sweep, True, False)
            for copy in dem_copies:
                copy.start()
        send_supply(sweep, False, True)
        for t in range(tiles):
            state = jnp.maximum(state, merge(sweep, t))
            reply(t)
        if sweep == 0:
            msg_ref[1, :, lanes:lanes + 128] = flag_row(state)
            state = jnp.zeros((8, 128), f32)
            wait_rows(n_sec - 1, lanes, dem_recv)
        relative = prices_row(sweep)
        if sweep == 0:
            sums = []
            for t in range(tiles):
                scale = relative[:, t * 128:(t + 1) * 128] * prod_row

                def next_step(i, acc, t=t, scale=scale):
                    rows = rows_of(i)
                    mass = live_ref[t, rows, :]
                    value = jnp.where(mass > 0.0,
                                      scale * col_ref[POW, rows, :] + best_ref[t, rows, :],
                                      0.3 * col_ref[CAP, rows, :])
                    val_ref[t, rows, :] = value
                    return acc + weigh(mass, rows, value)

                sums.append(lax.fori_loop(0, steps, next_step, jnp.zeros((8, 128), f32), unroll=16))
    rel_ref[...] = relative
    early = jnp.max(gat_ref[1, :, lanes:lanes + 128], axis=0, keepdims=True)
    flag_ref[0] = jnp.max(jnp.maximum(state, jnp.where(early > 0.0, 3.0, 0.0))).astype(jnp.int32)
    report = pltpu.make_async_copy(flag_ref, flag_hbm, in_sem.at[0])
    report.start()
    for t in range(tiles):
        scale = relative[:, t * 128:(t + 1) * 128] * prod_row

        def last_step(i, carry, t=t, scale=scale):
            rows = rows_of(i)
            out_ref[t, pl.ds(i, 8, stride=pitch), :] = jnp.where(
                live_ref[t, rows, :] > 0.0, scale * col_ref[POW, rows, :] + best_ref[t, rows, :],
                0.3 * col_ref[CAP, rows, :])
            return carry

        lax.fori_loop(0, steps, last_step, 0, unroll=8)
    cand_ref[...] = pays_ref[SWEEPS - 1]
    for sweep in range(SWEEPS):
        wait_rows(n_dev - 1, lanes + 128, msg_send.at[sweep])
        for t in range(tiles):
            pltpu.make_async_copy(pay_view(sweep, t), pay_view(sweep, t), pay_send.at[sweep, t]).wait()
    wait_rows(n_sec - 1, lanes, dem_send)
    report.wait()


def pruned_sweeps(start_value, firm_mass, survive, exit_index, demand, transition, install_cost):
    n_sec, n_cap = lax.axis_size("sector"), lax.axis_size("cap")
    sec_dev, prods, cap_dev = start_value.shape
    lanes = sec_dev * prods
    tiles = lanes // 128
    n_dev = n_sec * n_cap
    far = pl.BlockSpec(memory_space=pl.ANY)
    vmem = pl.BlockSpec(memory_space=pltpu.VMEM)
    smem = pl.BlockSpec(memory_space=pltpu.SMEM)
    f32 = jnp.float32
    dma = pltpu.SemaphoreType.DMA
    pack = max(RANGES, MERGED_RANGES)
    return pl.pallas_call(
        functools.partial(sweeps_kernel, n_sec, n_cap),
        out_shape=(
            jax.ShapeDtypeStruct((tiles, cap_dev + 64, 128), f32),
            jax.ShapeDtypeStruct((tiles, cap_dev, 128), f32),
            jax.ShapeDtypeStruct((tiles, 2, n_cap * SLOTS, 128), f32),
            jax.ShapeDtypeStruct((1, lanes), f32),
            jax.ShapeDtypeStruct((1,), jnp.int32),
        ),
        in_specs=[far] * 7,
        out_specs=(vmem, vmem, vmem, vmem, far),
        scratch_shapes=[
            pltpu.VMEM(start_value.shape, f32),
            pltpu.VMEM(start_value.shape, f32),
            pltpu.VMEM(start_value.shape, jnp.int32),
            pltpu.SMEM((sec_dev,), jnp.int32),
            pltpu.SMEM((sec_dev,), f32),
            pltpu.VMEM((prods, prods), f32),
            pltpu.VMEM((1, cap_dev), f32),
            pltpu.VMEM((tiles, cap_dev + 64, 128), f32),
            pltpu.VMEM((tiles, cap_dev + 64, 128), f32),
            pltpu.VMEM((tiles, cap_dev, 128), f32),
            pltpu.VMEM((tiles, cap_dev, 128), f32),
            pltpu.VMEM((tiles, RANGES, cap_dev, 128), f32),
            pltpu.VMEM((tiles, RANGES + 1, 8, 128), f32),
            pltpu.VMEM((MERGED_RANGES, n_cap * SLOTS, 128), f32),
            pltpu.VMEM((tiles, cap_dev, 128), f32),
            pltpu.VMEM((5, cap_dev, 128), f32),
            pltpu.VMEM((RANGES + 1, cap_dev, 128), f32),
            pltpu.VMEM((256, 256), jnp.bfloat16),
            pltpu.VMEM((128, 128), jnp.bfloat16),
            pltpu.VMEM((pack + 1, 8, 128), f32),
            pltpu.VMEM((3, CHUNK_SLOTS * 8, 128), f32),
            pltpu.VMEM((3, max(MERGED, n_cap * SLOTS), 128), f32),
            pltpu.VMEM((tiles * 8, 128), f32),
            pltpu.VMEM((n_sec, lanes), f32),
            pltpu.VMEM((SWEEPS, 1, lanes + 128), f32),
            pltpu.VMEM((SWEEPS, n_dev, lanes + 128), f32),
            pltpu.VMEM((1, lanes), f32),
            pltpu.VMEM((n_sec, lanes), f32),
            pltpu.VMEM((SWEEPS, tiles, 2, SLOTS, 128), f32),
            pltpu.VMEM((SWEEPS, tiles, 2, n_cap * SLOTS, 128), f32),
            pltpu.VMEM((n_dev - 1, 1, lanes + 128), f32),
            pltpu.SMEM((1,), jnp.int32),
            dma((7,)),
            dma((SWEEPS,)), dma((SWEEPS,)), dma, dma,
            dma((SWEEPS, tiles)), dma((SWEEPS, tiles)),
        ],
        compiler_params=pltpu.CompilerParams(
            collective_id=0, has_side_effects=True, vmem_limit_bytes=48 * 1024 * 1024
        ),
    )(start_value, firm_mass, survive, exit_index, demand, transition, install_cost[None, :])


def all_candidates(values, candidates, relative, survive, exit_index):
    sec_dev, prods, cap_dev = values.shape
    total = cap_dev * lax.axis_size("cap")
    capital = capital_of(lax.axis_index("cap") * cap_dev + jnp.arange(cap_dev, dtype=jnp.int32), total)
    prod_index = jnp.arange(prods, dtype=jnp.int32)
    output = jnp.exp(-0.5 + prod_index.astype(jnp.float32) / (prods - 1))[:, None] * capital[None, :] ** 0.6
    live = (survive == 1) & (prod_index[None, :, None] >= exit_index[:, None, None])
    flat = jnp.moveaxis(candidates, 0, 2).reshape(2, candidates.shape[2], sec_dev, prods)

    def one(best, pair):
        return jnp.maximum(best, pair[0][:, :, None] - pair[1][:, :, None] / capital), None

    moved, _ = lax.scan(one, jnp.full(values.shape, NEG, jnp.float32), (flat[0], flat[1]))
    again = relative[:, None, None] * output + (moved - 1.41 * capital)
    return jnp.where(live, jnp.maximum(values, again), values)


def group_sweep(gains, relative, survive, exit_index):
    sec_dev, prods, cap_dev = survive.shape
    tiles = gains.shape[0]
    total = cap_dev * lax.axis_size("cap")
    row_first = lax.axis_index("cap") * cap_dev
    capital = capital_of(row_first + jnp.arange(cap_dev, dtype=jnp.int32), total)
    prod_index = jnp.arange(prods, dtype=jnp.int32)
    output = jnp.exp(-0.5 + prod_index.astype(jnp.float32) / (prods - 1))[:, None] * capital[None, :] ** 0.6
    live = (survive == 1) & (prod_index[None, :, None] >= exit_index[:, None, None])
    natural = gains.reshape(tiles, cap_dev // 8, 8, 128).swapaxes(1, 2).reshape(tiles, cap_dev, 128)
    forward_value = natural.swapaxes(1, 2).reshape(sec_dev, prods, cap_dev) - 0.8 * capital
    rows = jnp.moveaxis(gather_blocks(forward_value, "cap"), 0, 2).reshape(sec_dev * prods, total)
    best = best_reply(rows, row_first, cap_dev).reshape(sec_dev, prods, cap_dev)
    return jnp.where(live, relative[:, None, None] * output + best, 0.3 * capital)


def finish_kernel(flipped_ref, row_ref, out_ref, rel_ref):
    tile_sec, prods, cap_dev = out_ref.shape
    lanes, sec_dev = row_ref.shape[1], rel_ref.shape[1]
    steps = cap_dev // 8
    for at in range(0, cap_dev, 128):
        spots = [(at + up) // steps * (steps + 8) for up in range(0, 128, steps)]
        block = jnp.concatenate([flipped_ref[0, spot:spot + steps, :] for spot in spots], axis=0)
        out_ref[:, :, at:at + 128] = block.T.reshape(tile_sec, prods, 128)

    @pl.when(pl.program_id(0) == 0)
    def _():
        column = jnp.sum(jnp.where(
            lax.broadcasted_iota(jnp.int32, (sec_dev, lanes), 1) == prods * lax.broadcasted_iota(
                jnp.int32, (sec_dev, lanes), 0), row_ref[...], 0.0), axis=1, keepdims=True)
        spot = lax.broadcasted_iota(jnp.int32, (sec_dev, sec_dev), 0) == lax.broadcasted_iota(
            jnp.int32, (sec_dev, sec_dev), 1)
        rel_ref[...] = jnp.sum(jnp.where(spot, column, 0.0), axis=0, keepdims=True)


def finish(flipped, row, sec_dev, prods):
    tiles, padded, _ = flipped.shape
    cap_dev = padded - 64
    values, relative = pl.pallas_call(
        finish_kernel,
        grid=(tiles,),
        out_shape=(jax.ShapeDtypeStruct((sec_dev, prods, cap_dev), jnp.float32),
                   jax.ShapeDtypeStruct((1, sec_dev), jnp.float32)),
        in_specs=[pl.BlockSpec((1, padded, 128), lambda t: (t, 0, 0)),
                  pl.BlockSpec(row.shape, lambda t: (0, 0))],
        out_specs=(pl.BlockSpec((sec_dev // tiles, prods, cap_dev), lambda t: (t, 0, 0)),
                   pl.BlockSpec((1, sec_dev), lambda t: (0, 0))),
    )(flipped, row)
    return values, relative[0]


def on_device(start_value, firm_mass, survive, exit_index, demand, transition, install_cost):
    args = (start_value, firm_mass, survive, exit_index, demand, transition, install_cost)
    sec_dev, prods, cap_dev = start_value.shape
    if 128 % prods or prods % 8 or sec_dev * prods % 128 or cap_dev % 128 or min(
            lax.axis_size("sector"), lax.axis_size("cap")) < 2:
        return dense_sweeps(*args)
    flipped, gains, candidates, row, state = pruned_sweeps(*args)

    def plain():
        return finish(flipped, row, sec_dev, prods)

    def wide():
        values, relative = plain()
        return all_candidates(values, candidates, relative, survive, exit_index), relative

    def group():
        relative = row.reshape(sec_dev, prods)[:, 0]
        return group_sweep(gains, relative, survive, exit_index), relative

    return lax.switch(state[0], (plain, wide, group, lambda: dense_sweeps(*args)))


def solution(mesh):
    return jax.shard_map(
        on_device,
        mesh=mesh,
        in_specs=(
            P("sector", None, "cap"),
            P("sector", None, "cap"),
            P("sector", None, "cap"),
            P("sector"),
            P("sector"),
            P(),
            P("cap"),
        ),
        out_specs=(P("sector", None, "cap"), P("sector")),
        check_vma=False,
    )
```
